32 devices in a mesh: dp: 16 (over z, x, core), rows: 2 (over y).
Axes of the slice: x: 2, y: 2, z: 4, core: 2. Of those that a mesh axis runs over, the one named last changes fastest.
Arguments:
- fine_level: bfloat16 [16, 32, 64, 256], P('dp', 'rows'), may hold values from -6 to 6
- out_grad: bfloat16 [16, 32, 64, 256], P('dp', 'rows'), may hold values from -6 to 6
- fine_input: bfloat16 [16, 32, 64, 256], P('dp', 'rows'), may hold values from -6 to 6
- mid_input: bfloat16 [16, 16, 32, 512], P('dp', None, None, 'rows'), may hold values from -6 to 6
- top_input: bfloat16 [16, 8, 16, 1024], P('dp', None, None, 'rows'), may hold values from -6 to 6
- smooth_weight: bfloat16 [3, 3, 256, 256], replicated, may hold values from -0.125 to 0.125
- fine_lateral: bfloat16 [256, 256], replicated, may hold values from -0.375 to 0.375
- mid_lateral: bfloat16 [512, 256], P('rows'), may hold values from -0.375 to 0.375
- top_lateral: bfloat16 [1024, 256], P('rows'), may hold values from -0.375 to 0.375
Outputs:
- grad_fine: bfloat16 [16, 32, 64, 256], P('dp', 'rows')
- grad_mid: bfloat16 [16, 16, 32, 512], P('dp', None, None, 'rows')
- grad_top: bfloat16 [16, 8, 16, 1024], P('dp', None, None, 'rows')
- kernel_grads: float32 [2560, 256], P('dp')
- midlat_grad: float32 [512, 256], P('rows')
- toplat_grad: float32 [1024, 256], P('rows')
The draws below stay inside these ranges and needn't reach their ends.
All inputs are finite; a program needn't handle non-finite values.
Results may differ from the reference program's by a relative error of at most 0.0062.
Values may be sent and summed in bfloat16 or wider, within the bound.
A program may use at most 64 MiB of HBM per device.

```python
import jax
import jax.numpy as jnp
from jax import lax

FPN = 256
C2 = 256
C3 = 512
C4 = 1024
W2 = 64
BATCH = 16
H2 = 32
H3 = 16
W3 = 32
H4 = 8
W4 = 16


def block_levels(rng, extent, split, smallest, top_value):
    def one(axis_at, shards_of):
        draws = jax.random.uniform(jax.random.fold_in(jax.random.fold_in(rng, 6), axis_at), (shards_of,), jnp.float32, smallest / len(split), top_value / len(split))
        return jnp.repeat(jnp.exp(draws), extent[axis_at] // shards_of).reshape((-1,) + (1,) * (len(extent) - axis_at - 1))

    loudness = one(*split[0])
    for cut in split[1:]:
        loudness = loudness * one(*cut)
    return loudness


def scatter_about(stream_key, shape, spread, bound, cuts=(), held_as=jnp.bfloat16):
    level = block_levels(stream_key, shape, cuts, -0.22, 0.18) if cuts else 1.0
    result = jax.random.normal(stream_key, shape, jnp.float32) * spread * level
    return jnp.minimum(jnp.maximum(result, -bound), bound).astype(held_as)


def setup_inputs(seed: int = 0) -> dict:
    streams_of = jax.random.split(jax.random.key(seed), 10)
    fine_level = scatter_about(streams_of[0], (BATCH, H2, W2, FPN), 1.0, 6.0, ((0, 16), (1, 2)))
    out_grad = scatter_about(streams_of[1], (BATCH, H2, W2, FPN), 1.0, 6.0, ((0, 16), (1, 2)))
    fine_input = scatter_about(streams_of[2], (BATCH, H2, W2, C2), 1.0, 6.0, ((0, 16), (1, 2)))
    mid_input = scatter_about(streams_of[3], (BATCH, H3, W3, C3), 1.0, 6.0, ((0, 16), (3, 2)))
    top_input = scatter_about(streams_of[4], (BATCH, H4, W4, C4), 1.0, 6.0, ((0, 16), (3, 2)))
    smooth_weight = scatter_about(streams_of[5], (3, 3, FPN, FPN), (9 * FPN) ** -0.5, 0.125)
    fine_lateral = scatter_about(streams_of[6], (C2, FPN), FPN ** -0.5, 0.375)
    mid_lateral = scatter_about(streams_of[7], (C3, FPN), FPN ** -0.5, 0.375, ((0, 2),))
    top_lateral = scatter_about(streams_of[8], (C4, FPN), FPN ** -0.5, 0.375, ((0, 2),))
    return dict(fine_level=fine_level, out_grad=out_grad, fine_input=fine_input, mid_input=mid_input, top_input=top_input, smooth_weight=smooth_weight, fine_lateral=fine_lateral, mid_lateral=mid_lateral, top_lateral=top_lateral)


def pool_two(field):
    rows_n, cols_n, chans = field.shape
    return field.reshape(rows_n // 2, 2, cols_n // 2, 2, chans).sum(axis=(1, 3))


def contract_last(left, right):
    return lax.dot_general(left, right, (((1,), (1,)), ((), ())), preferred_element_type=jnp.float32)


def contract_first(left, right):
    return lax.dot_general(left, right, (((0,), (0,)), ((), ())), preferred_element_type=jnp.float32)


def one_image(fine_map, grad_map, fine_in, mid_in, top_in, smooth_weight, fine_lateral, mid_lateral, top_lateral):
    height, width, chans = grad_map.shape
    cells = height * width
    padded = jnp.pad(grad_map, ((1, 1), (1, 1), (0, 0)))
    fine_flat = fine_map.reshape(cells, chans)
    level_grad = jnp.zeros((cells, chans), jnp.float32)
    pieces = []
    for tap_a in range(3):
        for tap_b in range(3):
            shifted = padded[2 - tap_a:2 - tap_a + height, 2 - tap_b:2 - tap_b + width, :].reshape(cells, chans)
            level_grad = level_grad + contract_last(shifted, smooth_weight[tap_a, tap_b])
            pieces.append(contract_first(fine_flat, shifted))
    fine_grad = level_grad.astype(jnp.bfloat16)
    grad_fine = contract_last(fine_grad, fine_lateral).astype(jnp.bfloat16).reshape(height, width, -1)
    pieces.append(contract_first(fine_in.reshape(cells, -1), fine_grad))
    kernel_term = jnp.concatenate(pieces, axis=0)
    mid_grad = pool_two(level_grad.reshape(height, width, chans)).astype(jnp.bfloat16)
    top_grad = pool_two(mid_grad.astype(jnp.float32)).astype(jnp.bfloat16)
    mid_flat = mid_grad.reshape(-1, chans)
    top_flat = top_grad.reshape(-1, chans)
    grad_mid = contract_last(mid_flat, mid_lateral).astype(jnp.bfloat16).reshape(mid_in.shape)
    grad_top = contract_last(top_flat, top_lateral).astype(jnp.bfloat16).reshape(top_in.shape)
    mid_term = contract_first(mid_in.reshape(mid_flat.shape[0], -1), mid_flat)
    top_term = contract_first(top_in.reshape(top_flat.shape[0], -1), top_flat)
    return grad_fine, grad_mid, grad_top, kernel_term, mid_term, top_term


def reference(fine_level, out_grad, fine_input, mid_input, top_input, smooth_weight, fine_lateral, mid_lateral, top_lateral):
    def step(carry, items):
        outs = one_image(items[0], items[1], items[2], items[3], items[4], smooth_weight, fine_lateral, mid_lateral, top_lateral)
        carry = (carry[0] + outs[3], carry[1] + outs[4], carry[2] + outs[5])
        return carry, (outs[0], outs[1], outs[2])

    start = (jnp.zeros((9 * FPN + C2, FPN), jnp.float32), jnp.zeros((C3, FPN), jnp.float32), jnp.zeros((C4, FPN), jnp.float32))
    sums, grads = lax.scan(step, start, (fine_level, out_grad, fine_input, mid_input, top_input))
    return grads[0], grads[1], grads[2], sums[0], sums[1], sums[2]
```

```python
import functools

import jax
import jax.numpy as jnp
from jax import lax
from jax.experimental import pallas as pl
from jax.experimental.pallas import tpu as pltpu
from jax.sharding import PartitionSpec as P

BF = jnp.bfloat16
F32 = jnp.float32
MESH = pl.DeviceIdType.MESH


def with_halo(value, sides, width):
    for axis, dim in sides:
        count, length = (lax.axis_size(axis), value.shape[dim])
        up = [(i, (i + 1) % count) for i in range(count - 1)]
        down = [(j, i) for i, j in up]
        last = lax.slice_in_dim(value, length - width, length, axis=dim)
        leading = lax.slice_in_dim(value, 0, width, axis=dim)
        before = lax.ppermute(last, axis, up)
        after = lax.ppermute(leading, axis, down)
        value = jnp.concatenate([before, value, after], axis=dim)
    return value


def pool_two(field):
    images, rows_n, cols_n, chans = field.shape
    return field.reshape(images, rows_n // 2, 2, cols_n // 2, 2, chans).sum(axis=(2, 4))


def contract_last(left, right):
    return lax.dot_general(
        left, right, (((1,), (1,)), ((), ())), preferred_element_type=jnp.float32
    )


def contract_first(left, right):
    return lax.dot_general(
        left, right, (((0,), (0,)), ((), ())), preferred_element_type=jnp.float32
    )


def plain_body(
    fine_level,
    out_grad,
    fine_input,
    mid_input,
    top_input,
    smooth_weight,
    fine_lateral,
    mid_lateral,
    top_lateral,
):
    images, strip, width, chans = out_grad.shape
    cells = images * strip * width
    rimmed = with_halo(out_grad, (("rows", 1),), 1)
    rimmed = jnp.pad(rimmed, ((0, 0), (0, 0), (1, 1), (0, 0)))
    fine_flat = fine_level.reshape(cells, chans)
    level_grad = jnp.zeros((cells, chans), jnp.float32)
    pieces = []
    for tap_a in range(3):
        for tap_b in range(3):
            shifted = rimmed[
                :, 2 - tap_a : 2 - tap_a + strip, 2 - tap_b : 2 - tap_b + width, :
            ].reshape(cells, chans)
            level_grad = level_grad + contract_last(shifted, smooth_weight[tap_a, tap_b])
            pieces.append(contract_first(fine_flat, shifted))
    fine_grad = level_grad.astype(jnp.bfloat16)
    grad_fine = (
        contract_last(fine_grad, fine_lateral)
        .astype(jnp.bfloat16)
        .reshape(images, strip, width, -1)
    )
    pieces.append(contract_first(fine_input.reshape(cells, -1), fine_grad))
    kernel_term = jnp.concatenate(pieces, axis=0)
    share = lax.psum_scatter(kernel_term, "dp", scatter_dimension=0, tiled=True)
    kernel_grads = lax.psum(share, "rows")
    pooled = pool_two(level_grad.reshape(images, strip, width, chans)).astype(jnp.bfloat16)
    mid_grad = lax.all_gather(pooled, "rows", axis=1, tiled=True)
    top_grad = pool_two(mid_grad.astype(jnp.float32)).astype(jnp.bfloat16)
    mid_flat = mid_grad.reshape(-1, chans)
    top_flat = top_grad.reshape(-1, chans)
    grad_mid = contract_last(mid_flat, mid_lateral).astype(jnp.bfloat16).reshape(mid_input.shape)
    grad_top = contract_last(top_flat, top_lateral).astype(jnp.bfloat16).reshape(top_input.shape)
    mid_term = contract_first(mid_input.reshape(mid_flat.shape[0], -1), mid_flat)
    top_term = contract_first(top_input.reshape(top_flat.shape[0], -1), top_flat)
    midlat_grad, toplat_grad = lax.psum((mid_term, top_term), "dp")
    return (grad_fine, grad_mid, grad_top, kernel_grads, midlat_grad, toplat_grad)


def rows_of(start, size, step):
    return pl.ds(pl.multiple_of(start, step), size)


def fused(
    nz, nx, nr, strip, width,
    fl_h, og_h, fi_h, mi_h, ti_h, w_h, lf_h, lm_h, lt_h,
    gf_h, gm_h, gt_h, kf_h, ga_h,
    og, fine, fin, mid_in, top_in, wcat, lat_f, lat_m, lat_t,
    halo, taps, ftr, acc, kacc, fg, pool_f, midg, topf, topg,
    kgb, ra, sb, rb, tb, rc, kf,
    ct, rca, sc, rcs, gath,
    gf, gm, gt,
    in_sem, w_sem, out_sem, halo_s, halo_r, mid_s, mid_r,
    a_s, a_r, b_s, b_r, c_s, c_r, d_s, d_r,
    ca_s, ca_r, cs_s, cs_r, cg_s, cg_r, cc_s, cc_r,
):
    chips = nz * nx
    d = lax.axis_index("dp")
    r = lax.axis_index("rows")
    core = lax.rem(d, 2)
    q = d // 2
    x = lax.rem(q, nx)
    z = q // nx
    other = 1 - core
    sibling = (q * 2 + other, r)
    cells, chans = og.shape
    share = kf.shape[0]
    part = share // nr

    def dev(z1, x1, r1):
        return ((z1 * nx + x1) * 2 + core, r1)

    def remote(src, dst, ss, rs, to):
        return pltpu.make_async_remote_copy(
            src_ref=src, dst_ref=dst, send_sem=ss, recv_sem=rs,
            device_id=to, device_id_type=MESH,
        )

    loads = []
    for n, (src, dst) in enumerate(
        ((og_h, og), (fl_h, fine.at[pl.ds(width, cells)]), (fi_h, fin), (lf_h, lat_f),
         (mi_h, mid_in), (ti_h, top_in), (lm_h, lat_m), (lt_h, lat_t))
    ):
        loads.append(pltpu.make_async_copy(src, dst, in_sem.at[n]))
    wloads = []
    for a in range(3):
        for b in range(3):
            wloads.append(pltpu.make_async_copy(
                w_h.at[a, b], wcat.at[a, :, b * chans:(b + 1) * chans], w_sem.at[3 * a + b]
            ))
    loads[0].start()
    for cp in wloads:
        cp.start()
    for cp in loads[1:]:
        cp.start()

    barrier = pltpu.get_barrier_semaphore()
    plane = [(i, j) for i in range(nx) for j in range(nr) if (i, j) != (0, 0)]
    greet = [sibling]
    for k in range(1, chips):
        greet.append((lax.rem(q + k, chips) * 2 + core, r))
    for i, j in plane:
        if j:
            greet.append(dev(z, lax.rem(x + i, nx), lax.rem(r + j, nr)))
    for to in greet:
        pl.semaphore_signal(barrier, inc=1, device_id=to, device_id_type=MESH)

    top_rim, low_rim = pl.ds(0, width), pl.ds((strip + 1) * width, width)
    taps[top_rim, :] = jnp.zeros((width, 3 * chans), BF)
    taps[low_rim, :] = jnp.zeros((width, 3 * chans), BF)
    fine[top_rim, :] = jnp.zeros((width, chans), BF)
    fine[low_rim, :] = jnp.zeros((width, chans), BF)

    col = lax.broadcasted_iota(jnp.int32, (width, chans), 0)

    def spread(value, here):
        wide = value.astype(F32)
        after = jnp.where(col == width - 1, 0.0, pltpu.roll(wide, width - 1, 0))
        before = jnp.where(col == 0, 0.0, pltpu.roll(wide, 1, 0))
        taps[here, 0:chans] = after.astype(BF)
        taps[here, chans:2 * chans] = value
        taps[here, 2 * chans:3 * chans] = before.astype(BF)

    loads[0].wait()
    pl.semaphore_wait(barrier, len(greet))
    down = remote(og.at[pl.ds(cells - width, width)], halo.at[0], halo_s.at[0], halo_r.at[0],
                  (d, lax.rem(r + 1, nr)))
    up = remote(og.at[pl.ds(0, width)], halo.at[1], halo_s.at[1], halo_r.at[1],
                (d, lax.rem(r + nr - 1, nr)))

    @pl.when(r < nr - 1)
    def _():
        down.start()

    @pl.when(r > 0)
    def _():
        up.start()

    def spread_row(y, carry):
        spread(og[rows_of(y * width, width, width), :], rows_of((y + 1) * width, width, width))
        return carry

    lax.fori_loop(0, strip, spread_row, 0)
    for cp in wloads:
        cp.wait()

    level = contract_last(taps[pl.ds(2 * width, cells), :], wcat[0])
    level += contract_last(taps[pl.ds(width, cells), :], wcat[1])
    level += contract_last(taps[pl.ds(0, cells), :], wcat[2])
    acc[...] = level

    half = width // 2
    mine = cells // 4
    lanes = [pl.ds(v * 128, 128) for v in range(chans // 128)]

    def pool(y0, count):
        for y in range(y0, y0 + count):
            pair = acc[pl.ds(2 * y * width, width), :] + acc[pl.ds((2 * y + 1) * width, width), :]
            for v in range(chans // 128):
                pool_f[v, pl.ds(y * width, width), :] = pair[:, v * 128:(v + 1) * 128]
        for v, lane in enumerate(lanes):
            midg[r, pl.ds(y0 * half, count * half), lane] = (
                pool_f[v, pl.ds(y0 * width, count * half, stride=2), :]
                + pool_f[v, pl.ds(y0 * width + 1, count * half, stride=2), :]
            ).astype(BF)

    mrows = strip // 2
    pool(1, mrows - 2)
    mids = []

    def send_mid(e, y0, count):
        here = midg.at[r, pl.ds(y0 * half, count * half)]
        for j in range(1, nr):
            cp = remote(here, here, mid_s.at[j - 1, e], mid_r.at[j - 1, e],
                        (d, lax.rem(r + j, nr)))
            cp.start()
            mids.append(cp)

    send_mid(0, 1, mrows - 2)

    inner = pl.ds(width, cells - 2 * width)
    fg[inner, :] = acc[inner, :].astype(BF)

    loads[1].wait()
    wide_t = fine[...].T
    ftr[pl.ds(0, chans), :] = wide_t[:, 0:cells]
    ftr[pl.ds(chans, chans), :] = fine[pl.ds(width, cells), :].T
    ftr[pl.ds(2 * chans, chans), :] = wide_t[:, 2 * width:2 * width + cells]

    def ktap(b, carry):
        got = jnp.dot(
            ftr[...], taps[pl.ds(width, cells), pl.ds(pl.multiple_of(b * chans, 128), chans)],
            preferred_element_type=F32,
        )
        kacc[0, rows_of(b * chans, chans, 16), :] = got[0:chans]
        kgb[rows_of((3 + b) * chans, chans, 16), :] = got[chans:2 * chans].astype(BF)
        kacc[1, rows_of(b * chans, chans, 16), :] = got[2 * chans:3 * chans]
        return carry

    lax.fori_loop(0, 3, ktap, 0)

    loads[2].wait()
    fsum = jnp.dot(fin[inner, :].T, fg[inner, :], preferred_element_type=F32)

    @pl.when(r > 0)
    def _():
        down.wait_recv()

    @pl.when(r == 0)
    def _():
        halo[0] = jnp.zeros_like(halo[0])

    @pl.when(r < nr - 1)
    def _():
        up.wait_recv()

    @pl.when(r == nr - 1)
    def _():
        halo[1] = jnp.zeros_like(halo[1])

    spread(halo[0], top_rim)
    spread(halo[1], low_rim)
    first, last = pl.ds(0, width), pl.ds(cells - width, width)
    acc[first, :] += contract_last(taps[top_rim, :], wcat[2])
    acc[last, :] += contract_last(taps[low_rim, :], wcat[0])
    pool(0, 1)
    pool(mrows - 1, 1)
    send_mid(1, 0, 1)
    send_mid(2, mrows - 1, 1)
    fg[first, :] = acc[first, :].astype(BF)
    fg[last, :] = acc[last, :].astype(BF)
    rim0 = jnp.dot(fine[pl.ds(cells, width), :].T, taps[low_rim, :], preferred_element_type=F32)
    rim2 = jnp.dot(fine[pl.ds(width, width), :].T, taps[top_rim, :], preferred_element_type=F32)
    for b in range(3):
        lane = slice(b * chans, (b + 1) * chans)
        kgb[pl.ds(b * chans, chans), :] = (kacc[0, pl.ds(b * chans, chans), :] + rim0[:, lane]).astype(BF)
        kgb[pl.ds((6 + b) * chans, chans), :] = (
            kacc[1, pl.ds(b * chans, chans), :] + rim2[:, lane]).astype(BF)
    fsum += jnp.dot(fin[first, :].T, fg[first, :], preferred_element_type=F32)
    fsum += jnp.dot(fin[last, :].T, fg[last, :], preferred_element_type=F32)
    kgb[pl.ds(9 * chans, fin.shape[1]), :] = fsum.astype(BF)

    low = z < nz // 2
    far = []
    for k in range(nz - 1):
        down_z = nz - 1 - k
        zt = jnp.where(low, jnp.where(down_z > z, down_z, down_z - 1), jnp.where(k < z, k, k + 1))
        far.append(zt)
    far.append(z)
    firsts = []
    for zt in far:
        for i in range(nx):
            n = zt * nx + i
            cp = remote(kgb.at[rows_of((2 * n + other) * share, share, 16)], ra.at[n],
                        a_s.at[n], a_r.at[n], sibling)
            cp.start()
            firsts.append((n, cp))

    loads[3].wait()
    gf[...] = contract_last(fg[...], lat_f[...]).astype(BF)
    outs = [pltpu.make_async_copy(gf, gf_h, out_sem.at[0])]
    outs[0].start()

    seconds = []
    for g, zt in enumerate(far):
        for n, cp in firsts[g * nx:(g + 1) * nx]:
            cp.wait_recv()
            sb[n] = (
                kgb[rows_of((2 * n + core) * share, share, 16), :].astype(F32) + ra[n].astype(F32)
            ).astype(BF)
        row = []
        for n, (i, j) in enumerate(plane):
            xt, rt = lax.rem(x + i, nx), lax.rem(r + j, nr)
            cp = remote(sb.at[zt * nx + xt, rows_of(rt * part, part, 16)], rb.at[n, g],
                        b_s.at[n, g], b_r.at[n, g], dev(z, xt, rt))
            cp.start()
            row.append(cp)
        seconds.append((g, zt, row))

    for cp in mids:
        cp.wait_recv()
    loads[4].wait()
    loads[5].wait()
    hw = half
    for t in range(nr):
        for y in range(strip // 4):
            pair = (
                midg[t, pl.ds(2 * y * hw, hw), :].astype(F32)
                + midg[t, pl.ds((2 * y + 1) * hw, hw), :].astype(F32)
            )
            for v in range(chans // 128):
                topf[v, pl.ds((t * (strip // 4) + y) * hw, hw), :] = pair[:, v * 128:(v + 1) * 128]
    tops = topg.shape[0]
    for v, lane in enumerate(lanes):
        topg[:, lane] = (
            topf[v, pl.ds(0, tops, stride=2), :] + topf[v, pl.ds(1, tops, stride=2), :]
        ).astype(BF)
    mflat = midg[...].reshape(nr * mine, chans)
    mc, tc = mid_in.shape[1], top_in.shape[1]
    ct[pl.ds(0, mc), :] = jnp.dot(
        mid_in[...].T, mflat, preferred_element_type=F32).astype(BF)
    ct[pl.ds(mc, tc), :] = jnp.dot(
        top_in[...].T, topg[...], preferred_element_type=F32).astype(BF)
    per = sc.shape[0]
    chunk = per // chips
    cfirst = remote(ct.at[rows_of(other * per, per, 16)], rca, ca_s, ca_r, sibling)
    cfirst.start()
    cfirst.wait_recv()
    sc[...] = (
        ct[rows_of(core * per, per, 16), :].astype(F32) + rca[...].astype(F32)
    ).astype(BF)
    cscat = []
    for k in range(1, chips):
        to = lax.rem(q + k, chips)
        cp = remote(sc.at[rows_of(to * chunk, chunk, 16)], rcs.at[k - 1],
                    cs_s.at[k - 1], cs_r.at[k - 1], (to * 2 + core, r))
        cp.start()
        cscat.append(cp)

    loads[6].wait()
    gm[...] = contract_last(mflat, lat_m[...]).astype(BF)
    outs.append(pltpu.make_async_copy(gm, gm_h, out_sem.at[1]))
    outs[1].start()
    loads[7].wait()
    gt[...] = contract_last(topg[...], lat_t[...]).astype(BF)
    outs.append(pltpu.make_async_copy(gt, gt_h, out_sem.at[2]))
    outs[2].start()

    thirds = []
    for g, zt, row in seconds[:-1]:
        total = sb[zt * nx + x, rows_of(r * part, part, 16), :].astype(F32)
        for n, cp in enumerate(row):
            cp.wait_recv()
            total += rb[n, g].astype(F32)
        tb[g] = total.astype(BF)
        cp = remote(tb.at[g], rc.at[z], c_s.at[g], c_r.at[z], dev(zt, x, r))
        cp.start()
        thirds.append(cp)

    total = sc[rows_of(q * chunk, chunk, 16), :].astype(F32)
    for k in range(1, chips):
        cscat[k - 1].wait_recv()
        total += rcs[k - 1].astype(F32)
    place = core * per + q * chunk
    gath[rows_of(place, chunk, 16), :] = total.astype(BF)
    cgath = []
    for k in range(1, chips):
        here = rows_of(place, chunk, 16)
        cp = remote(gath.at[here], gath.at[here], cg_s.at[k - 1], cg_r.at[k - 1],
                    (lax.rem(q + k, chips) * 2 + core, r))
        cp.start()
        cgath.append(cp)

    total = sb[z * nx + x, rows_of(r * part, part, 16), :].astype(F32)
    for n, cp in enumerate(seconds[-1][2]):
        cp.wait_recv()
        total += rb[n, nz - 1].astype(F32)
    for k in range(1, nz):
        source = lax.rem(z + k, nz)
        remote(tb.at[0], rc.at[source], c_s.at[0], c_r.at[source], dev(source, x, r)).wait_recv()
        total += rc[source].astype(F32)
    spot = rows_of(r * part, part, 16)
    kf[spot, :] = total.astype(BF)
    lasts = []
    for j in range(1, nr):
        cp = remote(kf.at[spot], kf.at[spot], d_s.at[j - 1], d_r.at[j - 1],
                    (d, lax.rem(r + j, nr)))
        cp.start()
        lasts.append(cp)

    for cp in cgath:
        cp.wait_recv()
    block = rows_of(core * per, per, 16)
    ccore = remote(gath.at[block], gath.at[block], cc_s, cc_r, sibling)
    ccore.start()
    for cp in lasts:
        cp.wait_recv()
    outs.append(pltpu.make_async_copy(kf, kf_h, out_sem.at[3]))
    outs[3].start()
    ccore.wait_recv()
    outs.append(pltpu.make_async_copy(gath, ga_h, out_sem.at[4]))
    outs[4].start()

    @pl.when(r < nr - 1)
    def _():
        down.wait_send()

    @pl.when(r > 0)
    def _():
        up.wait_send()

    sent = mids + [cp for _, cp in firsts] + [cfirst] + cscat + cgath + thirds + lasts + [ccore]
    for _, _, row in seconds:
        sent += row
    for cp in sent:
        cp.wait_send()
    for cp in outs:
        cp.wait()


def put_out(gf_i, gm_i, gt_i, kf_i, ga_i, gf_o, gm_o, gt_o, kg_o, ml_o, tl_o,
            kf, ga, kg, ml, tl, in_sem, out_sem):
    loads = [
        pltpu.make_async_copy(src, dst, in_sem.at[n])
        for n, (src, dst) in enumerate(
            ((ga_i, ga), (kf_i, kf)))
    ]
    for cp in loads:
        cp.start()
    stores = [
        pltpu.make_async_copy(src, dst, out_sem.at[n])
        for n, (src, dst) in enumerate(
            ((gf_i, gf_o), (gm_i, gm_o), (gt_i, gt_o), (kg, kg_o), (ml, ml_o), (tl, tl_o)))
    ]
    for n in range(3):
        stores[n].start()
    loads[1].wait()
    kg[...] = kf[...].astype(F32)
    stores[3].start()
    loads[0].wait()
    mc = ml.shape[0]
    ml[...] = ga[pl.ds(0, mc), :].astype(F32)
    stores[4].start()
    tl[...] = ga[pl.ds(mc, tl.shape[0]), :].astype(F32)
    stores[5].start()
    for cp in stores:
        cp.wait()


def kernel_body(nz, nx, nr, fine_level, out_grad, fine_input, mid_input, top_input,
                smooth_weight, fine_lateral, mid_lateral, top_lateral):
    _, strip, width, chans = out_grad.shape
    cells = strip * width
    cin = fine_input.shape[-1]
    mc, tc = mid_input.shape[-1], top_input.shape[-1]
    mcells = mid_input.shape[1] * mid_input.shape[2]
    tcells = top_input.shape[1] * top_input.shape[2]
    chips = nz * nx
    rows = 9 * chans + cin
    share = rows // (2 * chips)
    part = share // nr
    per = (mc + tc) // 2
    chunk = per // chips
    npl = nx * nr - 1
    dma = pltpu.SemaphoreType.DMA
    vm = pltpu.VMEM
    scratch = [
        vm((cells, chans), BF), vm(((strip + 2) * width, chans), BF), vm((cells, cin), BF),
        vm((mcells, mc), BF), vm((tcells, tc), BF), vm((3, chans, 3 * chans), BF),
        vm((cin, chans), BF), vm((mc, chans), BF), vm((tc, chans), BF),
        vm((2, width, chans), BF), vm(((strip + 2) * width, 3 * chans), BF),
        vm((3 * chans, cells), BF), vm((cells, chans), F32), vm((2, 3 * chans, chans), F32), vm((cells, chans), BF), vm((chans // 128, cells // 2, 128), F32),
        vm((nr, cells // 4, chans), BF), vm((chans // 128, mcells // 2, 128), F32), vm((tcells, chans), BF),
        vm((rows, chans), BF), vm((chips, share, chans), BF), vm((chips, share, chans), BF),
        vm((npl, nz, part, chans), BF), vm((nz - 1, part, chans), BF),
        vm((nz, part, chans), BF), vm((share, chans), BF),
        vm((2 * per, chans), BF), vm((per, chans), BF), vm((per, chans), BF),
        vm((chips - 1, chunk, chans), BF), vm((2 * per, chans), BF),
        vm((cells, cin), BF), vm((mcells, mc), BF), vm((tcells, tc), BF),
        dma((8,)), dma((9,)), dma((5,)), dma((2,)), dma((2,)), dma((nr - 1, 3)), dma((nr - 1, 3)),
        dma((chips,)), dma((chips,)), dma((npl, nz)), dma((npl, nz)),
        dma((nz - 1,)), dma((nz,)), dma((nr - 1,)), dma((nr - 1,)),
        dma(()), dma(()), dma((chips - 1,)), dma((chips - 1,)),
        dma((chips - 1,)), dma((chips - 1,)), dma(()), dma(()),
    ]
    hbm = pl.BlockSpec(memory_space=pltpu.HBM)
    anyspec = pl.BlockSpec(memory_space=pl.ANY)
    wide = [
        jax.ShapeDtypeStruct((cells, cin), BF), jax.ShapeDtypeStruct((mcells, mc), BF),
        jax.ShapeDtypeStruct((tcells, tc), BF),
    ]
    held = [jax.ShapeDtypeStruct((share, chans), BF), jax.ShapeDtypeStruct((2 * per, chans), BF)]
    final = [
        jax.ShapeDtypeStruct((share, chans), F32), jax.ShapeDtypeStruct((mc, chans), F32),
        jax.ShapeDtypeStruct((tc, chans), F32),
    ]
    whole = 67043328
    between = pl.pallas_call(
        functools.partial(fused, nz, nx, nr, strip, width),
        out_shape=[pltpu.VMEM(o.shape, o.dtype) for o in wide + held],
        in_specs=[hbm] * 9,
        out_specs=[anyspec] * 5,
        scratch_shapes=scratch,
        compiler_params=pltpu.CompilerParams(
            collective_id=0, has_side_effects=True, vmem_limit_bytes=48 * 1024 * 1024
        ),
    )(*(pltpu.with_memory_space_constraint(value, pltpu.HBM) for value in (
        fine_level.reshape(cells, chans), out_grad.reshape(cells, chans),
        fine_input.reshape(cells, cin), mid_input.reshape(mcells, mc),
        top_input.reshape(tcells, tc), smooth_weight, fine_lateral, mid_lateral, top_lateral,
    )))
    gf, gm, gt, kg, ml, tl = pl.pallas_call(
        put_out,
        out_shape=wide + final,
        in_specs=[anyspec] * 5,
        out_specs=[hbm] * 6,
        scratch_shapes=[vm(o.shape, o.dtype) for o in held + final]
        + [dma((2,)), dma((6,))],
        compiler_params=pltpu.CompilerParams(vmem_limit_bytes=8 * 1024 * 1024),
    )(*between)
    return (
        gf.reshape(fine_input.shape), gm.reshape(mid_input.shape),
        gt.reshape(top_input.shape), kg, ml, tl,
    )


def body(nr, *args):
    fine_level, out_grad, fine_input, mid_input, top_input = args[:5]
    dp = lax.axis_size("dp")
    chips = dp // 2
    nx = max((n for n in range(1, chips + 1) if chips % n == 0 and n * n <= chips), default=1)
    images, strip, width, chans = out_grad.shape
    rows = 9 * chans + fine_input.shape[-1]
    coarse = mid_input.shape[-1] + top_input.shape[-1]
    fits = (
        dp % 2 == 0 and images == 1 and nr > 1 and chips > nx
        and rows % (dp * nr * 16) == 0 and coarse % (dp * 16) == 0
        and strip % 4 == 0 and strip >= 8 and width % 64 == 0 and chans % 128 == 0
    )
    if not fits:
        return plain_body(*args)
    return kernel_body(chips // nx, nx, nr, *args)


def solution(mesh):
    placed = (
        P("dp", "rows", None, None),
        P("dp", "rows", None, None),
        P("dp", "rows", None, None),
        P("dp", None, None, "rows"),
        P("dp", None, None, "rows"),
        P(),
        P(),
        P("rows", None),
        P("rows", None),
    )
    return jax.shard_map(
        functools.partial(body, mesh.shape["rows"]),
        mesh=mesh,
        in_specs=placed,
        out_specs=(
            P("dp", "rows", None, None),
            P("dp", None, None, "rows"),
            P("dp", None, None, "rows"),
            P("dp", None),
            P("rows", None),
            P("rows", None),
        ),
        check_vma=False,
    )
```

```python
import functools

import jax
import jax.numpy as jnp
from jax import lax
from jax.experimental import pallas as pl
from jax.experimental.pallas import tpu as pltpu
from jax.sharding import PartitionSpec as P

BF = jnp.bfloat16
F32 = jnp.float32
MESH = pl.DeviceIdType.MESH


def with_halo(value, sides, width):
    for axis, dim in sides:
        count, length = (lax.axis_size(axis), value.shape[dim])
        up = [(i, (i + 1) % count) for i in range(count - 1)]
        down = [(j, i) for i, j in up]
        last = lax.slice_in_dim(value, length - width, length, axis=dim)
        leading = lax.slice_in_dim(value, 0, width, axis=dim)
        before = lax.ppermute(last, axis, up)
        after = lax.ppermute(leading, axis, down)
        value = jnp.concatenate([before, value, after], axis=dim)
    return value


def pool_two(field):
    images, rows_n, cols_n, chans = field.shape
    return field.reshape(images, rows_n // 2, 2, cols_n // 2, 2, chans).sum(axis=(2, 4))


def contract_last(left, right):
    return lax.dot_general(
        left, right, (((1,), (1,)), ((), ())), preferred_element_type=jnp.float32
    )


def contract_first(left, right):
    return lax.dot_general(
        left, right, (((0,), (0,)), ((), ())), preferred_element_type=jnp.float32
    )


def plain_body(
    fine_level,
    out_grad,
    fine_input,
    mid_input,
    top_input,
    smooth_weight,
    fine_lateral,
    mid_lateral,
    top_lateral,
):
    images, strip, width, chans = out_grad.shape
    cells = images * strip * width
    rimmed = with_halo(out_grad, (("rows", 1),), 1)
    rimmed = jnp.pad(rimmed, ((0, 0), (0, 0), (1, 1), (0, 0)))
    fine_flat = fine_level.reshape(cells, chans)
    level_grad = jnp.zeros((cells, chans), jnp.float32)
    pieces = []
    for tap_a in range(3):
        for tap_b in range(3):
            shifted = rimmed[
                :, 2 - tap_a : 2 - tap_a + strip, 2 - tap_b : 2 - tap_b + width, :
            ].reshape(cells, chans)
            level_grad = level_grad + contract_last(shifted, smooth_weight[tap_a, tap_b])
            pieces.append(contract_first(fine_flat, shifted))
    fine_grad = level_grad.astype(jnp.bfloat16)
    grad_fine = (
        contract_last(fine_grad, fine_lateral)
        .astype(jnp.bfloat16)
        .reshape(images, strip, width, -1)
    )
    pieces.append(contract_first(fine_input.reshape(cells, -1), fine_grad))
    kernel_term = jnp.concatenate(pieces, axis=0)
    share = lax.psum_scatter(kernel_term, "dp", scatter_dimension=0, tiled=True)
    kernel_grads = lax.psum(share, "rows")
    pooled = pool_two(level_grad.reshape(images, strip, width, chans)).astype(jnp.bfloat16)
    mid_grad = lax.all_gather(pooled, "rows", axis=1, tiled=True)
    top_grad = pool_two(mid_grad.astype(jnp.float32)).astype(jnp.bfloat16)
    mid_flat = mid_grad.reshape(-1, chans)
    top_flat = top_grad.reshape(-1, chans)
    grad_mid = contract_last(mid_flat, mid_lateral).astype(jnp.bfloat16).reshape(mid_input.shape)
    grad_top = contract_last(top_flat, top_lateral).astype(jnp.bfloat16).reshape(top_input.shape)
    mid_term = contract_first(mid_input.reshape(mid_flat.shape[0], -1), mid_flat)
    top_term = contract_first(top_input.reshape(top_flat.shape[0], -1), top_flat)
    midlat_grad, toplat_grad = lax.psum((mid_term, top_term), "dp")
    return (grad_fine, grad_mid, grad_top, kernel_grads, midlat_grad, toplat_grad)


def rows_of(start, size, step):
    return pl.ds(pl.multiple_of(start, step), size)


def fused(
    nz, nx, nr, strip, width,
    fl_h, og_h, fi_h, mi_h, ti_h, w_h, lf_h, lm_h, lt_h,
    gf_h, gm_h, gt_h, kf_h, ga_h,
    og, fine, fin, mid_in, top_in, wcat, lat_f, lat_m, lat_t,
    halo, taps, ftr, acc, kacc, fg, pool_f, midg, topf, topg,
    kgb, ra, sb, rb, tb, rc, kf,
    ct, rca, sc, rcs, gath,
    gf, gm, gt,
    in_sem, w_sem, out_sem, halo_s, halo_r, mid_s, mid_r,
    a_s, a_r, b_s, b_r, c_s, c_r, d_s, d_r,
    ca_s, ca_r, cs_s, cs_r, cg_s, cg_r, cc_s, cc_r, relay,
):
    chips = nz * nx
    d = lax.axis_index("dp")
    r = lax.axis_index("rows")
    core = lax.rem(d, 2)
    q = d // 2
    x = lax.rem(q, nx)
    z = q // nx
    other = 1 - core
    sibling = (q * 2 + other, r)
    cells, chans = og.shape
    share = kf.shape[0]
    part = share // nr

    def dev(z1, x1, r1):
        return ((z1 * nx + x1) * 2 + core, r1)

    def remote(src, dst, ss, rs, to):
        return pltpu.make_async_remote_copy(
            src_ref=src, dst_ref=dst, send_sem=ss, recv_sem=rs,
            device_id=to, device_id_type=MESH,
        )

    loads = []
    for n, (src, dst) in enumerate(
        ((og_h, og), (fl_h, fine.at[pl.ds(width, cells)]), (fi_h, fin), (lf_h, lat_f),
         (mi_h, mid_in), (ti_h, top_in), (lm_h, lat_m), (lt_h, lat_t))
    ):
        loads.append(pltpu.make_async_copy(src, dst, in_sem.at[n]))
    wloads = []
    for a in range(3):
        for b in range(3):
            wloads.append(pltpu.make_async_copy(
                w_h.at[a, b], wcat.at[a, :, b * chans:(b + 1) * chans], w_sem.at[3 * a + b]
            ))
    loads[0].start()
    for cp in wloads:
        cp.start()
    for cp in loads[1:]:
        cp.start()

    barrier = pltpu.get_barrier_semaphore()
    plane = [(i, j) for i in range(nx) for j in range(nr) if (i, j) != (0, 0)]
    near = []
    for low_end, high_end, before, after in (
        (z > 0, z < nz - 1, dev(jnp.maximum(z - 1, 0), x, r), dev(jnp.minimum(z + 1, nz - 1), x, r)),
        (x > 0, x < nx - 1, dev(z, jnp.maximum(x - 1, 0), r), dev(z, jnp.minimum(x + 1, nx - 1), r)),
        (r > 0, r < nr - 1, dev(z, x, jnp.maximum(r - 1, 0)), dev(z, x, jnp.minimum(r + 1, nr - 1))),
    ):
        near += [(low_end, before), (high_end, after)]
    nearby = sum(there.astype(jnp.int32) for there, _ in near)

    def greet(sem):
        for there, to in near:
            @pl.when(there)
            def _():
                pl.semaphore_signal(sem, inc=1, device_id=to, device_id_type=MESH)

    def hear(k):
        pl.semaphore_wait(relay.at[k], nearby)
        if k + 1 < relays:
            greet(relay.at[k + 1])

    relays = relay.shape[0]
    pl.semaphore_signal(barrier, inc=1, device_id=sibling, device_id_type=MESH)
    greet(barrier)

    top_rim, low_rim = pl.ds(0, width), pl.ds((strip + 1) * width, width)
    taps[top_rim, :] = jnp.zeros((width, 3 * chans), BF)
    taps[low_rim, :] = jnp.zeros((width, 3 * chans), BF)
    fine[top_rim, :] = jnp.zeros((width, chans), BF)
    fine[low_rim, :] = jnp.zeros((width, chans), BF)

    col = lax.broadcasted_iota(jnp.int32, (width, chans), 0)

    def spread(value, here):
        wide = value.astype(F32)
        after = jnp.where(col == width - 1, 0.0, pltpu.roll(wide, width - 1, 0))
        before = jnp.where(col == 0, 0.0, pltpu.roll(wide, 1, 0))
        taps[here, 0:chans] = after.astype(BF)
        taps[here, chans:2 * chans] = value
        taps[here, 2 * chans:3 * chans] = before.astype(BF)

    loads[0].wait()
    def spread_row(y, carry):
        spread(og[rows_of(y * width, width, width), :], rows_of((y + 1) * width, width, width))
        return carry

    lax.fori_loop(0, strip, spread_row, 0)
    loads[1].wait()
    wide_t = fine[...].T
    ftr[pl.ds(0, chans), :] = wide_t[:, 0:cells]
    ftr[pl.ds(chans, chans), :] = fine[pl.ds(width, cells), :].T
    ftr[pl.ds(2 * chans, chans), :] = wide_t[:, 2 * width:2 * width + cells]

    pl.semaphore_wait(barrier, nearby + 1)
    greet(relay.at[0])
    down = remote(og.at[pl.ds(cells - width, width)], halo.at[0], halo_s.at[0], halo_r.at[0],
                  (d, lax.rem(r + 1, nr)))
    up = remote(og.at[pl.ds(0, width)], halo.at[1], halo_s.at[1], halo_r.at[1],
                (d, lax.rem(r + nr - 1, nr)))

    @pl.when(r < nr - 1)
    def _():
        down.start()

    @pl.when(r > 0)
    def _():
        up.start()

    for cp in wloads:
        cp.wait()

    level = contract_last(taps[pl.ds(2 * width, cells), :], wcat[0])
    level += contract_last(taps[pl.ds(width, cells), :], wcat[1])
    level += contract_last(taps[pl.ds(0, cells), :], wcat[2])
    acc[...] = level

    hear(0)
    half = width // 2
    mine = cells // 4
    lanes = [pl.ds(v * 128, 128) for v in range(chans // 128)]

    def pool(y0, count):
        for y in range(count):
            at = 2 * (y0 + y) * width
            pair = acc[rows_of(at, width, width), :] + acc[rows_of(at + width, width, width), :]
            for v in range(chans // 128):
                pool_f[v, pl.ds(y * width, width), :] = pair[:, v * 128:(v + 1) * 128]
        for v, lane in enumerate(lanes):
            midg[r, rows_of(y0 * half, count * half, 16), lane] = (
                pool_f[v, pl.ds(0, count * half, stride=2), :]
                + pool_f[v, pl.ds(1, count * half, stride=2), :]
            ).astype(BF)

    mrows = strip // 2
    pool(0, mrows)
    rims = [r] if nr == 2 else [0, 1]
    start = r if nr == 2 else 1
    count = mrows - len(rims)
    mids = []

    def send_mid(e, y0, count):
        here = midg.at[r, rows_of(y0 * half, count * half, 16)]
        for j in range(1, nr):
            cp = remote(here, here, mid_s.at[j - 1, e], mid_r.at[j - 1, e],
                        (d, lax.rem(r + j, nr)))
            cp.start()
            mids.append(cp)

    send_mid(0, start, count)
    inner = rows_of(start * width, cells - len(rims) * width, width)
    fg[...] = acc[...].astype(BF)

    def ktap(b, carry):
        got = jnp.dot(
            ftr[...], taps[pl.ds(width, cells), pl.ds(pl.multiple_of(b * chans, 128), chans)],
            preferred_element_type=F32,
        )
        for a in range(3):
            kgb[rows_of((3 * a + b) * chans, chans, 16), :] = got[a * chans:(a + 1) * chans].astype(BF)
        kacc[0, rows_of(b * chans, chans, 16), :] = got[0:chans]
        kacc[1, rows_of(b * chans, chans, 16), :] = got[2 * chans:3 * chans]
        return carry

    lax.fori_loop(0, 3, ktap, 0)

    hear(1)
    loads[2].wait()
    fsum = jnp.dot(fin[inner, :].T, fg[inner, :], preferred_element_type=F32)

    @pl.when(r > 0)
    def _():
        down.wait_recv()

    @pl.when(r < nr - 1)
    def _():
        up.wait_recv()

    if nr > 2:
        @pl.when(r == 0)
        def _():
            halo[0] = jnp.zeros_like(halo[0])

        @pl.when(r == nr - 1)
        def _():
            halo[1] = jnp.zeros_like(halo[1])

    def mend(n, e):
        rim = rows_of((1 - e) * (strip + 1) * width, width, width)
        edge = rows_of((1 - e) * (cells - width), width, width)
        mate = rows_of((1 - e) * (cells - width) + width, width, width)
        y0 = (1 - e) * (mrows - 1)
        spread(halo[1 - e], rim)
        acc[edge, :] += contract_last(taps[rim, :], wcat[2 * e])
        pool(y0, 1)
        send_mid(1 + n, y0, 1)
        fg[edge, :] = acc[edge, :].astype(BF)
        more = jnp.dot(fine[mate, :].T, taps[rim, :], preferred_element_type=F32)
        for b in range(3):
            kgb[rows_of((6 * e + b) * chans, chans, 16), :] = (
                kacc[e, pl.ds(b * chans, chans), :] + more[:, b * chans:(b + 1) * chans]
            ).astype(BF)
        return edge

    for n, e in enumerate(rims):
        edge = mend(n, e)
        fsum += jnp.dot(fin[edge, :].T, fg[edge, :], preferred_element_type=F32)
    kgb[pl.ds(9 * chans, fin.shape[1]), :] = fsum.astype(BF)

    for k in range(2, relays):
        hear(k)
    low = z < nz // 2
    far = []
    for k in range(nz - 1):
        down_z = nz - 1 - k
        zt = jnp.where(low, jnp.where(down_z > z, down_z, down_z - 1), jnp.where(k < z, k, k + 1))
        far.append(zt)
    far.append(z)
    firsts = []
    for zt in far:
        for i in range(nx):
            n = zt * nx + i
            cp = remote(kgb.at[rows_of((2 * n + other) * share, share, 16)], ra.at[n],
                        a_s.at[n], a_r.at[n], sibling)
            cp.start()
            firsts.append((n, cp))

    loads[3].wait()
    gf[...] = contract_last(fg[...], lat_f[...]).astype(BF)
    outs = [pltpu.make_async_copy(gf, gf_h, out_sem.at[0])]
    outs[0].start()

    seconds = []

    def sum_group(g):
        for n, cp in firsts[g * nx:(g + 1) * nx]:
            cp.wait_recv()
            sb[n] = (
                kgb[rows_of((2 * n + core) * share, share, 16), :].astype(F32) + ra[n].astype(F32)
            ).astype(BF)

    def send_group(g):
        row = []
        for n, (i, j) in enumerate(plane):
            xt, rt = lax.rem(x + i, nx), lax.rem(r + j, nr)
            cp = remote(sb.at[far[g] * nx + xt, rows_of(rt * part, part, 16)], rb.at[n, g],
                        b_s.at[n, g], b_r.at[n, g], dev(z, xt, rt))
            cp.start()
            row.append(cp)
        seconds.append((g, far[g], row))

    ahead = nz // 2
    for g in range(ahead):
        sum_group(g)
        send_group(g)

    for cp in mids:
        cp.wait_recv()
    loads[4].wait()
    loads[5].wait()
    hw = half
    for t in range(nr):
        for y in range(strip // 4):
            pair = (
                midg[t, pl.ds(2 * y * hw, hw), :].astype(F32)
                + midg[t, pl.ds((2 * y + 1) * hw, hw), :].astype(F32)
            )
            for v in range(chans // 128):
                topf[v, pl.ds((t * (strip // 4) + y) * hw, hw), :] = pair[:, v * 128:(v + 1) * 128]
    tops = topg.shape[0]
    for v, lane in enumerate(lanes):
        topg[:, lane] = (
            topf[v, pl.ds(0, tops, stride=2), :] + topf[v, pl.ds(1, tops, stride=2), :]
        ).astype(BF)
    mflat = midg[...].reshape(nr * mine, chans)
    mc, tc = mid_in.shape[1], top_in.shape[1]
    ct[pl.ds(0, mc), :] = jnp.dot(
        mid_in[...].T, mflat, preferred_element_type=F32).astype(BF)
    ct[pl.ds(mc, tc), :] = jnp.dot(
        top_in[...].T, topg[...], preferred_element_type=F32).astype(BF)
    per = sc.shape[0]
    chunk = per // chips
    cfirst = remote(ct.at[rows_of(other * per, per, 16)], rca, ca_s, ca_r, sibling)
    cfirst.start()
    for g in range(ahead, nz):
        sum_group(g)
    cfirst.wait_recv()
    sc[...] = (
        ct[rows_of(core * per, per, 16), :].astype(F32) + rca[...].astype(F32)
    ).astype(BF)
    cscat = []
    for k in range(1, chips):
        to = lax.rem(q + k, chips)
        cp = remote(sc.at[rows_of(to * chunk, chunk, 16)], rcs.at[k - 1],
                    cs_s.at[k - 1], cs_r.at[k - 1], (to * 2 + core, r))
        cp.start()
        cscat.append(cp)

    for g in range(ahead, nz):
        send_group(g)

    loads[6].wait()
    gm[...] = contract_last(mflat, lat_m[...]).astype(BF)
    outs.append(pltpu.make_async_copy(gm, gm_h, out_sem.at[1]))
    outs[1].start()
    loads[7].wait()
    gt[...] = contract_last(topg[...], lat_t[...]).astype(BF)
    outs.append(pltpu.make_async_copy(gt, gt_h, out_sem.at[2]))
    outs[2].start()

    thirds = []
    for g, zt, row in seconds[:-1]:
        total = sb[zt * nx + x, rows_of(r * part, part, 16), :].astype(F32)
        for n, cp in enumerate(row):
            cp.wait_recv()
            total += rb[n, g].astype(F32)
        tb[g] = total.astype(BF)
        cp = remote(tb.at[g], rc.at[z], c_s.at[g], c_r.at[z], dev(zt, x, r))
        cp.start()
        thirds.append(cp)

    total = sc[rows_of(q * chunk, chunk, 16), :].astype(F32)
    for k in range(1, chips):
        cscat[k - 1].wait_recv()
        total += rcs[k - 1].astype(F32)
    place = core * per + q * chunk
    gath[rows_of(place, chunk, 16), :] = total.astype(BF)
    cgath = []
    for k in range(1, chips):
        here = rows_of(place, chunk, 16)
        cp = remote(gath.at[here], gath.at[here], cg_s.at[k - 1], cg_r.at[k - 1],
                    (lax.rem(q + k, chips) * 2 + core, r))
        cp.start()
        cgath.append(cp)

    total = sb[z * nx + x, rows_of(r * part, part, 16), :].astype(F32)
    for n, cp in enumerate(seconds[-1][2]):
        cp.wait_recv()
        total += rb[n, nz - 1].astype(F32)
    for k in range(1, nz):
        source = lax.rem(z + k, nz)
        remote(tb.at[0], rc.at[source], c_s.at[0], c_r.at[source], dev(source, x, r)).wait_recv()
        total += rc[source].astype(F32)
    spot = rows_of(r * part, part, 16)
    kf[spot, :] = total.astype(BF)
    lasts = []
    for j in range(1, nr):
        cp = remote(kf.at[spot], kf.at[spot], d_s.at[j - 1], d_r.at[j - 1],
                    (d, lax.rem(r + j, nr)))
        cp.start()
        lasts.append(cp)

    for cp in cgath:
        cp.wait_recv()
    block = rows_of(core * per, per, 16)
    ccore = remote(gath.at[block], gath.at[block], cc_s, cc_r, sibling)
    ccore.start()
    for cp in lasts:
        cp.wait_recv()
    outs.append(pltpu.make_async_copy(kf, kf_h, out_sem.at[3]))
    outs[3].start()
    ccore.wait_recv()
    outs.append(pltpu.make_async_copy(gath, ga_h, out_sem.at[4]))
    outs[4].start()

    @pl.when(r < nr - 1)
    def _():
        down.wait_send()

    @pl.when(r > 0)
    def _():
        up.wait_send()

    sent = mids + [cp for _, cp in firsts] + [cfirst] + cscat + cgath + thirds + lasts + [ccore]
    for _, _, row in seconds:
        sent += row
    for cp in sent:
        cp.wait_send()
    for cp in outs:
        cp.wait()


def put_out(gf_i, gm_i, gt_i, kf_i, ga_i, gf_o, gm_o, gt_o, kg_o, ml_o, tl_o,
            kf, ga, kg, ml, tl, in_sem, out_sem):
    loads = [
        pltpu.make_async_copy(src, dst, in_sem.at[n])
        for n, (src, dst) in enumerate(
            ((ga_i, ga), (kf_i, kf)))
    ]
    for cp in loads:
        cp.start()
    stores = [
        pltpu.make_async_copy(src, dst, out_sem.at[n])
        for n, (src, dst) in enumerate(
            ((gf_i, gf_o), (gm_i, gm_o), (gt_i, gt_o), (kg, kg_o), (ml, ml_o), (tl, tl_o)))
    ]
    for n in range(3):
        stores[n].start()
    loads[1].wait()
    kg[...] = kf[...].astype(F32)
    stores[3].start()
    loads[0].wait()
    mc = ml.shape[0]
    ml[...] = ga[pl.ds(0, mc), :].astype(F32)
    stores[4].start()
    tl[...] = ga[pl.ds(mc, tl.shape[0]), :].astype(F32)
    stores[5].start()
    for cp in stores:
        cp.wait()


def kernel_body(nz, nx, nr, fine_level, out_grad, fine_input, mid_input, top_input,
                smooth_weight, fine_lateral, mid_lateral, top_lateral):
    _, strip, width, chans = out_grad.shape
    cells = strip * width
    cin = fine_input.shape[-1]
    mc, tc = mid_input.shape[-1], top_input.shape[-1]
    mcells = mid_input.shape[1] * mid_input.shape[2]
    tcells = top_input.shape[1] * top_input.shape[2]
    chips = nz * nx
    rows = 9 * chans + cin
    share = rows // (2 * chips)
    part = share // nr
    per = (mc + tc) // 2
    chunk = per // chips
    npl = nx * nr - 1
    dma = pltpu.SemaphoreType.DMA
    vm = pltpu.VMEM
    scratch = [
        vm((cells, chans), BF), vm(((strip + 2) * width, chans), BF), vm((cells, cin), BF),
        vm((mcells, mc), BF), vm((tcells, tc), BF), vm((3, chans, 3 * chans), BF),
        vm((cin, chans), BF), vm((mc, chans), BF), vm((tc, chans), BF),
        vm((2, width, chans), BF), vm(((strip + 2) * width, 3 * chans), BF),
        vm((3 * chans, cells), BF), vm((cells, chans), F32), vm((2, 3 * chans, chans), F32), vm((cells, chans), BF), vm((chans // 128, cells // 2, 128), F32),
        vm((nr, cells // 4, chans), BF), vm((chans // 128, mcells // 2, 128), F32), vm((tcells, chans), BF),
        vm((rows, chans), BF), vm((chips, share, chans), BF), vm((chips, share, chans), BF),
        vm((npl, nz, part, chans), BF), vm((nz - 1, part, chans), BF),
        vm((nz, part, chans), BF), vm((share, chans), BF),
        vm((2 * per, chans), BF), vm((per, chans), BF), vm((per, chans), BF),
        vm((chips - 1, chunk, chans), BF), vm((2 * per, chans), BF),
        vm((cells, cin), BF), vm((mcells, mc), BF), vm((tcells, tc), BF),
        dma((8,)), dma((9,)), dma((5,)), dma((2,)), dma((2,)), dma((nr - 1, 3)), dma((nr - 1, 3)),
        dma((chips,)), dma((chips,)), dma((npl, nz)), dma((npl, nz)),
        dma((nz - 1,)), dma((nz,)), dma((nr - 1,)), dma((nr - 1,)),
        dma(()), dma(()), dma((chips - 1,)), dma((chips - 1,)),
        dma((chips - 1,)), dma((chips - 1,)), dma(()), dma(()),
        pltpu.SemaphoreType.REGULAR((max(nz + nx, nx + nr) - 3,)),
    ]
    hbm = pl.BlockSpec(memory_space=pltpu.HBM)
    anyspec = pl.BlockSpec(memory_space=pl.ANY)
    wide = [
        jax.ShapeDtypeStruct((cells, cin), BF), jax.ShapeDtypeStruct((mcells, mc), BF),
        jax.ShapeDtypeStruct((tcells, tc), BF),
    ]
    held = [jax.ShapeDtypeStruct((share, chans), BF), jax.ShapeDtypeStruct((2 * per, chans), BF)]
    final = [
        jax.ShapeDtypeStruct((share, chans), F32), jax.ShapeDtypeStruct((mc, chans), F32),
        jax.ShapeDtypeStruct((tc, chans), F32),
    ]
    whole = 67043328
    between = pl.pallas_call(
        functools.partial(fused, nz, nx, nr, strip, width),
        out_shape=[pltpu.VMEM(o.shape, o.dtype) for o in wide + held],
        in_specs=[hbm] * 9,
        out_specs=[anyspec] * 5,
        scratch_shapes=scratch,
        compiler_params=pltpu.CompilerParams(
            collective_id=0, has_side_effects=True, vmem_limit_bytes=48 * 1024 * 1024
        ),
    )(*(pltpu.with_memory_space_constraint(value, pltpu.HBM) for value in (
        fine_level.reshape(cells, chans), out_grad.reshape(cells, chans),
        fine_input.reshape(cells, cin), mid_input.reshape(mcells, mc),
        top_input.reshape(tcells, tc), smooth_weight, fine_lateral, mid_lateral, top_lateral,
    )))
    gf, gm, gt, kg, ml, tl = pl.pallas_call(
        put_out,
        out_shape=wide + final,
        in_specs=[anyspec] * 5,
        out_specs=[hbm] * 6,
        scratch_shapes=[vm(o.shape, o.dtype) for o in held + final]
        + [dma((2,)), dma((6,))],
        compiler_params=pltpu.CompilerParams(vmem_limit_bytes=8 * 1024 * 1024),
    )(*between)
    return (
        gf.reshape(fine_input.shape), gm.reshape(mid_input.shape),
        gt.reshape(top_input.shape), kg, ml, tl,
    )


def body(nr, *args):
    fine_level, out_grad, fine_input, mid_input, top_input = args[:5]
    dp = lax.axis_size("dp")
    chips = dp // 2
    nx = max((n for n in range(1, chips + 1) if chips % n == 0 and n * n <= chips), default=1)
    images, strip, width, chans = out_grad.shape
    rows = 9 * chans + fine_input.shape[-1]
    coarse = mid_input.shape[-1] + top_input.shape[-1]
    fits = (
        dp % 2 == 0 and images == 1 and nr > 1 and chips > nx > 1 and chips // nx > 2
        and rows % (dp * nr * 16) == 0 and coarse % (dp * 16) == 0
        and strip % 4 == 0 and strip >= 8 and width % 64 == 0 and chans % 128 == 0
    )
    if not fits:
        return plain_body(*args)
    return kernel_body(chips // nx, nx, nr, *args)


def solution(mesh):
    placed = (
        P("dp", "rows", None, None),
        P("dp", "rows", None, None),
        P("dp", "rows", None, None),
        P("dp", None, None, "rows"),
        P("dp", None, None, "rows"),
        P(),
        P(),
        P("rows", None),
        P("rows", None),
    )
    return jax.shard_map(
        functools.partial(body, mesh.shape["rows"]),
        mesh=mesh,
        in_specs=placed,
        out_specs=(
            P("dp", "rows", None, None),
            P("dp", None, None, "rows"),
            P("dp", None, None, "rows"),
            P("dp", None),
            P("rows", None),
            P("rows", None),
        ),
        check_vma=False,
    )
```

```python
import functools

import jax
import jax.numpy as jnp
from jax import lax
from jax.experimental import pallas as pl
from jax.experimental.pallas import tpu as pltpu
from jax.sharding import PartitionSpec as P

BF = jnp.bfloat16
F32 = jnp.float32
MESH = pl.DeviceIdType.MESH


def with_halo(value, sides, width):
    for axis, dim in sides:
        count, length = (lax.axis_size(axis), value.shape[dim])
        up = [(i, (i + 1) % count) for i in range(count - 1)]
        down = [(j, i) for i, j in up]
        last = lax.slice_in_dim(value, length - width, length, axis=dim)
        leading = lax.slice_in_dim(value, 0, width, axis=dim)
        before = lax.ppermute(last, axis, up)
        after = lax.ppermute(leading, axis, down)
        value = jnp.concatenate([before, value, after], axis=dim)
    return value


def pool_two(field):
    images, rows_n, cols_n, chans = field.shape
    return field.reshape(images, rows_n // 2, 2, cols_n // 2, 2, chans).sum(axis=(2, 4))


def contract_last(left, right):
    return lax.dot_general(
        left, right, (((1,), (1,)), ((), ())), preferred_element_type=jnp.float32
    )


def contract_first(left, right):
    return lax.dot_general(
        left, right, (((0,), (0,)), ((), ())), preferred_element_type=jnp.float32
    )


def plain_body(
    fine_level,
    out_grad,
    fine_input,
    mid_input,
    top_input,
    smooth_weight,
    fine_lateral,
    mid_lateral,
    top_lateral,
):
    images, strip, width, chans = out_grad.shape
    cells = images * strip * width
    rimmed = with_halo(out_grad, (("rows", 1),), 1)
    rimmed = jnp.pad(rimmed, ((0, 0), (0, 0), (1, 1), (0, 0)))
    fine_flat = fine_level.reshape(cells, chans)
    level_grad = jnp.zeros((cells, chans), jnp.float32)
    pieces = []
    for tap_a in range(3):
        for tap_b in range(3):
            shifted = rimmed[
                :, 2 - tap_a : 2 - tap_a + strip, 2 - tap_b : 2 - tap_b + width, :
            ].reshape(cells, chans)
            level_grad = level_grad + contract_last(shifted, smooth_weight[tap_a, tap_b])
            pieces.append(contract_first(fine_flat, shifted))
    fine_grad = level_grad.astype(jnp.bfloat16)
    grad_fine = (
        contract_last(fine_grad, fine_lateral)
        .astype(jnp.bfloat16)
        .reshape(images, strip, width, -1)
    )
    pieces.append(contract_first(fine_input.reshape(cells, -1), fine_grad))
    kernel_term = jnp.concatenate(pieces, axis=0)
    share = lax.psum_scatter(kernel_term, "dp", scatter_dimension=0, tiled=True)
    kernel_grads = lax.psum(share, "rows")
    pooled = pool_two(level_grad.reshape(images, strip, width, chans)).astype(jnp.bfloat16)
    mid_grad = lax.all_gather(pooled, "rows", axis=1, tiled=True)
    top_grad = pool_two(mid_grad.astype(jnp.float32)).astype(jnp.bfloat16)
    mid_flat = mid_grad.reshape(-1, chans)
    top_flat = top_grad.reshape(-1, chans)
    grad_mid = contract_last(mid_flat, mid_lateral).astype(jnp.bfloat16).reshape(mid_input.shape)
    grad_top = contract_last(top_flat, top_lateral).astype(jnp.bfloat16).reshape(top_input.shape)
    mid_term = contract_first(mid_input.reshape(mid_flat.shape[0], -1), mid_flat)
    top_term = contract_first(top_input.reshape(top_flat.shape[0], -1), top_flat)
    midlat_grad, toplat_grad = lax.psum((mid_term, top_term), "dp")
    return (grad_fine, grad_mid, grad_top, kernel_grads, midlat_grad, toplat_grad)


def rows_of(start, size, step):
    return pl.ds(pl.multiple_of(start, step), size)


def fused(
    nz, nx, nr, strip, width,
    fl_h, og_h, fi_h, mi_h, ti_h, w_h, lf_h, lm_h, lt_h,
    gf_h, gm_h, gt_h, kf_h, ga_h,
    og, fine, fin, mid_in, top_in, wcat, lat_f, lat_m, lat_t,
    halo, taps, ftr, acc, kacc, fg, pool_f, midg, topf, topg,
    kgb, ra, sb, rb, tb, rc, kf,
    ct, rca, sc, rcs, gath,
    in_sem, w_sem, halo_s, halo_r, mid_s, mid_r,
    a_s, a_r, b_s, b_r, c_s, c_r, d_s, d_r,
    ca_s, ca_r, cs_s, cs_r, cg_s, cg_r, cc_s, cc_r, relay,
):
    chips = nz * nx
    d = lax.axis_index("dp")
    r = lax.axis_index("rows")
    core = lax.rem(d, 2)
    q = d // 2
    x = lax.rem(q, nx)
    z = q // nx
    other = 1 - core
    sibling = (q * 2 + other, r)
    cells, chans = og.shape
    share = kf.shape[0]
    part = share // nr

    def dev(z1, x1, r1):
        return ((z1 * nx + x1) * 2 + core, r1)

    def remote(src, dst, ss, rs, to):
        return pltpu.make_async_remote_copy(
            src_ref=src, dst_ref=dst, send_sem=ss, recv_sem=rs,
            device_id=to, device_id_type=MESH,
        )

    loads = []
    for n, (src, dst) in enumerate(
        ((og_h, og), (fl_h, fine.at[pl.ds(width, cells)]), (fi_h, fin), (lf_h, lat_f),
         (mi_h, mid_in), (ti_h, top_in), (lm_h, lat_m), (lt_h, lat_t))
    ):
        loads.append(pltpu.make_async_copy(src, dst, in_sem.at[n]))
    wloads = []
    for a in range(3):
        for b in range(3):
            wloads.append(pltpu.make_async_copy(
                w_h.at[a, b], wcat.at[a, :, b * chans:(b + 1) * chans], w_sem.at[3 * a + b]
            ))
    loads[0].start()
    for cp in wloads:
        cp.start()
    for cp in loads[1:]:
        cp.start()

    barrier = pltpu.get_barrier_semaphore()
    plane = [(i, j) for i in range(nx) for j in range(nr) if (i, j) != (0, 0)]
    near = []
    for low_end, high_end, before, after in (
        (z > 0, z < nz - 1, dev(jnp.maximum(z - 1, 0), x, r), dev(jnp.minimum(z + 1, nz - 1), x, r)),
        (x > 0, x < nx - 1, dev(z, jnp.maximum(x - 1, 0), r), dev(z, jnp.minimum(x + 1, nx - 1), r)),
        (r > 0, r < nr - 1, dev(z, x, jnp.maximum(r - 1, 0)), dev(z, x, jnp.minimum(r + 1, nr - 1))),
    ):
        near += [(low_end, before), (high_end, after)]
    nearby = sum(there.astype(jnp.int32) for there, _ in near)

    def greet(sem):
        for there, to in near:
            @pl.when(there)
            def _():
                pl.semaphore_signal(sem, inc=1, device_id=to, device_id_type=MESH)

    def hear(k):
        pl.semaphore_wait(relay.at[k], nearby)
        if k + 1 < relays:
            greet(relay.at[k + 1])

    relays = relay.shape[0]
    pl.semaphore_signal(barrier, inc=1, device_id=sibling, device_id_type=MESH)
    greet(barrier)

    top_rim, low_rim = pl.ds(0, width), pl.ds((strip + 1) * width, width)
    taps[top_rim, :] = jnp.zeros((width, 3 * chans), BF)
    taps[low_rim, :] = jnp.zeros((width, 3 * chans), BF)
    fine[top_rim, :] = jnp.zeros((width, chans), BF)
    fine[low_rim, :] = jnp.zeros((width, chans), BF)

    col = lax.broadcasted_iota(jnp.int32, (width, chans), 0)

    def spread(value, here):
        wide = value.astype(F32)
        after = jnp.where(col == width - 1, 0.0, pltpu.roll(wide, width - 1, 0))
        before = jnp.where(col == 0, 0.0, pltpu.roll(wide, 1, 0))
        taps[here, 0:chans] = after.astype(BF)
        taps[here, chans:2 * chans] = value
        taps[here, 2 * chans:3 * chans] = before.astype(BF)

    loads[0].wait()
    def spread_row(y, carry):
        spread(og[rows_of(y * width, width, width), :], rows_of((y + 1) * width, width, width))
        return carry

    lax.fori_loop(0, strip, spread_row, 0)
    loads[1].wait()
    wide_t = fine[...].T
    ftr[pl.ds(0, chans), :] = wide_t[:, 0:cells]
    ftr[pl.ds(chans, chans), :] = fine[pl.ds(width, cells), :].T
    ftr[pl.ds(2 * chans, chans), :] = wide_t[:, 2 * width:2 * width + cells]

    pl.semaphore_wait(barrier, nearby + 1)
    greet(relay.at[0])
    down = remote(og.at[pl.ds(cells - width, width)], halo.at[0], halo_s.at[0], halo_r.at[0],
                  (d, lax.rem(r + 1, nr)))
    up = remote(og.at[pl.ds(0, width)], halo.at[1], halo_s.at[1], halo_r.at[1],
                (d, lax.rem(r + nr - 1, nr)))

    @pl.when(r < nr - 1)
    def _():
        down.start()

    @pl.when(r > 0)
    def _():
        up.start()

    for cp in wloads:
        cp.wait()

    level = contract_last(taps[pl.ds(2 * width, cells), :], wcat[0])
    level += contract_last(taps[pl.ds(width, cells), :], wcat[1])
    level += contract_last(taps[pl.ds(0, cells), :], wcat[2])
    acc[...] = level

    hear(0)
    half = width // 2
    mine = cells // 4
    lanes = [pl.ds(v * 128, 128) for v in range(chans // 128)]

    def pool(y0, count):
        for y in range(count):
            at = 2 * (y0 + y) * width
            pair = acc[rows_of(at, width, width), :] + acc[rows_of(at + width, width, width), :]
            for v in range(chans // 128):
                pool_f[v, pl.ds(y * width, width), :] = pair[:, v * 128:(v + 1) * 128]
        for v, lane in enumerate(lanes):
            midg[r, rows_of(y0 * half, count * half, 16), lane] = (
                pool_f[v, pl.ds(0, count * half, stride=2), :]
                + pool_f[v, pl.ds(1, count * half, stride=2), :]
            ).astype(BF)

    mrows = strip // 2
    pool(0, mrows)
    rims = [r] if nr == 2 else [0, 1]
    start = r if nr == 2 else 1
    count = mrows - len(rims)
    mids = []

    def send_mid(e, y0, count):
        here = midg.at[r, rows_of(y0 * half, count * half, 16)]
        for j in range(1, nr):
            cp = remote(here, here, mid_s.at[j - 1, e], mid_r.at[j - 1, e],
                        (d, lax.rem(r + j, nr)))
            cp.start()
            mids.append(cp)

    send_mid(0, start, count)
    inner = rows_of(start * width, cells - len(rims) * width, width)
    fg[...] = acc[...].astype(BF)

    def ktap(b, carry):
        got = jnp.dot(
            ftr[...], taps[pl.ds(width, cells), pl.ds(pl.multiple_of(b * chans, 128), chans)],
            preferred_element_type=F32,
        )
        for a in range(3):
            kgb[rows_of((3 * a + b) * chans, chans, 16), :] = got[a * chans:(a + 1) * chans].astype(BF)
        kacc[0, rows_of(b * chans, chans, 16), :] = got[0:chans]
        kacc[1, rows_of(b * chans, chans, 16), :] = got[2 * chans:3 * chans]
        return carry

    lax.fori_loop(0, 3, ktap, 0)

    hear(1)
    loads[2].wait()
    fsum = jnp.dot(fin[inner, :].T, fg[inner, :], preferred_element_type=F32)

    @pl.when(r > 0)
    def _():
        down.wait_recv()

    @pl.when(r < nr - 1)
    def _():
        up.wait_recv()

    if nr > 2:
        @pl.when(r == 0)
        def _():
            halo[0] = jnp.zeros_like(halo[0])

        @pl.when(r == nr - 1)
        def _():
            halo[1] = jnp.zeros_like(halo[1])

    def mend(n, e):
        rim = rows_of((1 - e) * (strip + 1) * width, width, width)
        edge = rows_of((1 - e) * (cells - width), width, width)
        mate = rows_of((1 - e) * (cells - width) + width, width, width)
        y0 = (1 - e) * (mrows - 1)
        spread(halo[1 - e], rim)
        acc[edge, :] += contract_last(taps[rim, :], wcat[2 * e])
        pool(y0, 1)
        send_mid(1 + n, y0, 1)
        fg[edge, :] = acc[edge, :].astype(BF)
        more = jnp.dot(fine[mate, :].T, taps[rim, :], preferred_element_type=F32)
        for b in range(3):
            kgb[rows_of((6 * e + b) * chans, chans, 16), :] = (
                kacc[e, pl.ds(b * chans, chans), :] + more[:, b * chans:(b + 1) * chans]
            ).astype(BF)
        return edge

    for n, e in enumerate(rims):
        edge = mend(n, e)
        fsum += jnp.dot(fin[edge, :].T, fg[edge, :], preferred_element_type=F32)
    kgb[pl.ds(9 * chans, fin.shape[1]), :] = fsum.astype(BF)

    for k in range(2, relays):
        hear(k)
    low = z < nz // 2
    far = []
    for k in range(nz - 1):
        down_z = nz - 1 - k
        zt = jnp.where(low, jnp.where(down_z > z, down_z, down_z - 1), jnp.where(k < z, k, k + 1))
        far.append(zt)
    far.append(z)
    firsts = []
    for zt in far:
        for i in range(nx):
            n = zt * nx + i
            cp = remote(kgb.at[rows_of((2 * n + other) * share, share, 16)], ra.at[n],
                        a_s.at[n], a_r.at[n], sibling)
            cp.start()
            firsts.append((n, cp))

    loads[3].wait()
    gf_h[...] = contract_last(fg[...], lat_f[...]).astype(BF)

    seconds = []

    def sum_group(g):
        for n, cp in firsts[g * nx:(g + 1) * nx]:
            cp.wait_recv()
            sb[n] = (
                kgb[rows_of((2 * n + core) * share, share, 16), :].astype(F32) + ra[n].astype(F32)
            ).astype(BF)

    def send_group(g):
        row = []
        for n, (i, j) in enumerate(plane):
            xt, rt = lax.rem(x + i, nx), lax.rem(r + j, nr)
            cp = remote(sb.at[far[g] * nx + xt, rows_of(rt * part, part, 16)], rb.at[n, g],
                        b_s.at[n, g], b_r.at[n, g], dev(z, xt, rt))
            cp.start()
            row.append(cp)
        seconds.append((g, far[g], row))

    ahead = nz - 1
    for g in range(ahead):
        sum_group(g)
        send_group(g)

    for cp in mids:
        cp.wait_recv()
    loads[4].wait()
    loads[5].wait()
    hw = half
    for t in range(nr):
        for y in range(strip // 4):
            pair = (
                midg[t, pl.ds(2 * y * hw, hw), :].astype(F32)
                + midg[t, pl.ds((2 * y + 1) * hw, hw), :].astype(F32)
            )
            for v in range(chans // 128):
                topf[v, pl.ds((t * (strip // 4) + y) * hw, hw), :] = pair[:, v * 128:(v + 1) * 128]
    tops = topg.shape[0]
    for v, lane in enumerate(lanes):
        topg[:, lane] = (
            topf[v, pl.ds(0, tops, stride=2), :] + topf[v, pl.ds(1, tops, stride=2), :]
        ).astype(BF)
    mflat = midg[...].reshape(nr * mine, chans)
    mc, tc = mid_in.shape[1], top_in.shape[1]
    ct[pl.ds(0, mc), :] = jnp.dot(
        mid_in[...].T, mflat, preferred_element_type=F32).astype(BF)
    ct[pl.ds(mc, tc), :] = jnp.dot(
        top_in[...].T, topg[...], preferred_element_type=F32).astype(BF)
    per = sc.shape[0]
    chunk = per // chips
    cfirst = remote(ct.at[rows_of(other * per, per, 16)], rca, ca_s, ca_r, sibling)
    cfirst.start()
    for g in range(ahead, nz):
        sum_group(g)
    cfirst.wait_recv()
    sc[...] = (
        ct[rows_of(core * per, per, 16), :].astype(F32) + rca[...].astype(F32)
    ).astype(BF)
    cscat = []
    for k in range(1, chips):
        to = lax.rem(q + k, chips)
        cp = remote(sc.at[rows_of(to * chunk, chunk, 16)], rcs.at[k - 1],
                    cs_s.at[k - 1], cs_r.at[k - 1], (to * 2 + core, r))
        cp.start()
        cscat.append(cp)

    for g in range(ahead, nz):
        send_group(g)

    loads[6].wait()
    gm_h[...] = contract_last(mflat, lat_m[...]).astype(BF)
    loads[7].wait()
    gt_h[...] = contract_last(topg[...], lat_t[...]).astype(BF)

    thirds = []
    for g, zt, row in seconds[:-1]:
        total = sb[zt * nx + x, rows_of(r * part, part, 16), :].astype(F32)
        for n, cp in enumerate(row):
            cp.wait_recv()
            total += rb[n, g].astype(F32)
        tb[g] = total.astype(BF)
        cp = remote(tb.at[g], rc.at[z], c_s.at[g], c_r.at[z], dev(zt, x, r))
        cp.start()
        thirds.append(cp)

    total = sc[rows_of(q * chunk, chunk, 16), :].astype(F32)
    for k in range(1, chips):
        cscat[k - 1].wait_recv()
        total += rcs[k - 1].astype(F32)
    place = core * per + q * chunk
    gath[rows_of(place, chunk, 16), :] = total.astype(BF)

    def hand_over(k):
        held = gath.at[rows_of(core * per + lax.rem(q + chips - k, chips) * chunk, chunk, 16)]
        return remote(held, held, cc_s.at[k], cc_r.at[k], sibling)

    cgath = []
    for k in range(1, chips):
        here = rows_of(place, chunk, 16)
        cp = remote(gath.at[here], gath.at[here], cg_s.at[k - 1], cg_r.at[k - 1],
                    (lax.rem(q + k, chips) * 2 + core, r))
        cp.start()
        cgath.append(cp)
    hand_over(0).start()

    total = sb[z * nx + x, rows_of(r * part, part, 16), :].astype(F32)
    for n, cp in enumerate(seconds[-1][2]):
        cp.wait_recv()
        total += rb[n, nz - 1].astype(F32)
    for k in range(1, nz):
        source = lax.rem(z + k, nz)
        remote(tb.at[0], rc.at[source], c_s.at[0], c_r.at[source], dev(source, x, r)).wait_recv()
        total += rc[source].astype(F32)
    spot = rows_of(r * part, part, 16)
    kf[spot, :] = total.astype(BF)
    lasts = []
    for j in range(1, nr):
        cp = remote(kf.at[spot], kf.at[spot], d_s.at[j - 1], d_r.at[j - 1],
                    (d, lax.rem(r + j, nr)))
        cp.start()
        lasts.append(cp)

    for k in range(1, chips):
        cgath[k - 1].wait_recv()
        hand_over(k).start()
    for cp in lasts:
        cp.wait_recv()
    kf_h[...] = kf[...].astype(F32)
    block = rows_of(core * per, per, 16)
    ga_h[block, :] = gath[block, :].astype(F32)
    for k in range(chips):
        hand_over(k).wait_recv()
    rest = rows_of(other * per, per, 16)
    ga_h[rest, :] = gath[rest, :].astype(F32)

    @pl.when(r < nr - 1)
    def _():
        down.wait_send()

    @pl.when(r > 0)
    def _():
        up.wait_send()

    sent = mids + [cp for _, cp in firsts] + [cfirst] + cscat + cgath + thirds + lasts + [hand_over(k) for k in range(chips)]
    for _, _, row in seconds:
        sent += row
    for cp in sent:
        cp.wait_send()


def put_out(gf_i, gm_i, gt_i, kg_i, ga_i, gf_o, gm_o, gt_o, kg_o, ml_o, tl_o, out_sem):
    mc = ml_o.shape[0]
    pairs = (
        (ga_i.at[pl.ds(mc, tl_o.shape[0])], tl_o), (gf_i, gf_o), (ga_i.at[pl.ds(0, mc)], ml_o),
        (gm_i, gm_o), (kg_i, kg_o), (gt_i, gt_o),
    )
    stores = [pltpu.make_async_copy(src, dst, out_sem.at[n]) for n, (src, dst) in enumerate(pairs)]
    for cp in stores:
        cp.start()
    for cp in stores:
        cp.wait()


def kernel_body(nz, nx, nr, fine_level, out_grad, fine_input, mid_input, top_input,
                smooth_weight, fine_lateral, mid_lateral, top_lateral):
    _, strip, width, chans = out_grad.shape
    cells = strip * width
    cin = fine_input.shape[-1]
    mc, tc = mid_input.shape[-1], top_input.shape[-1]
    mcells = mid_input.shape[1] * mid_input.shape[2]
    tcells = top_input.shape[1] * top_input.shape[2]
    chips = nz * nx
    rows = 9 * chans + cin
    share = rows // (2 * chips)
    part = share // nr
    per = (mc + tc) // 2
    chunk = per // chips
    npl = nx * nr - 1
    dma = pltpu.SemaphoreType.DMA
    vm = pltpu.VMEM
    scratch = [
        vm((cells, chans), BF), vm(((strip + 2) * width, chans), BF), vm((cells, cin), BF),
        vm((mcells, mc), BF), vm((tcells, tc), BF), vm((3, chans, 3 * chans), BF),
        vm((cin, chans), BF), vm((mc, chans), BF), vm((tc, chans), BF),
        vm((2, width, chans), BF), vm(((strip + 2) * width, 3 * chans), BF),
        vm((3 * chans, cells), BF), vm((cells, chans), F32), vm((2, 3 * chans, chans), F32), vm((cells, chans), BF), vm((chans // 128, cells // 2, 128), F32),
        vm((nr, cells // 4, chans), BF), vm((chans // 128, mcells // 2, 128), F32), vm((tcells, chans), BF),
        vm((rows, chans), BF), vm((chips, share, chans), BF), vm((chips, share, chans), BF),
        vm((npl, nz, part, chans), BF), vm((nz - 1, part, chans), BF),
        vm((nz, part, chans), BF), vm((share, chans), BF),
        vm((2 * per, chans), BF), vm((per, chans), BF), vm((per, chans), BF),
        vm((chips - 1, chunk, chans), BF), vm((2 * per, chans), BF),
        dma((8,)), dma((9,)), dma((2,)), dma((2,)), dma((nr - 1, 3)), dma((nr - 1, 3)),
        dma((chips,)), dma((chips,)), dma((npl, nz)), dma((npl, nz)),
        dma((nz - 1,)), dma((nz,)), dma((nr - 1,)), dma((nr - 1,)),
        dma(()), dma(()), dma((chips - 1,)), dma((chips - 1,)),
        dma((chips - 1,)), dma((chips - 1,)), dma((chips,)), dma((chips,)),
        pltpu.SemaphoreType.REGULAR((max(nz + nx, nx + nr) - 3,)),
    ]
    hbm = pl.BlockSpec(memory_space=pltpu.HBM)
    inner = pl.BlockSpec(memory_space=pltpu.VMEM)
    wide = [
        jax.ShapeDtypeStruct((cells, cin), BF), jax.ShapeDtypeStruct((mcells, mc), BF),
        jax.ShapeDtypeStruct((tcells, tc), BF),
    ]
    held = [jax.ShapeDtypeStruct((share, chans), F32), jax.ShapeDtypeStruct((2 * per, chans), F32)]
    final = [
        jax.ShapeDtypeStruct((share, chans), F32), jax.ShapeDtypeStruct((mc, chans), F32),
        jax.ShapeDtypeStruct((tc, chans), F32),
    ]
    whole = 67043328
    between = pl.pallas_call(
        functools.partial(fused, nz, nx, nr, strip, width),
        out_shape=[pltpu.VMEM(o.shape, o.dtype) for o in wide + held],
        in_specs=[hbm] * 9,
        out_specs=[inner] * 5,
        scratch_shapes=scratch,
        compiler_params=pltpu.CompilerParams(
            collective_id=0, has_side_effects=True, vmem_limit_bytes=48 * 1024 * 1024
        ),
    )(*(pltpu.with_memory_space_constraint(value, pltpu.HBM) for value in (
        fine_level.reshape(cells, chans), out_grad.reshape(cells, chans),
        fine_input.reshape(cells, cin), mid_input.reshape(mcells, mc),
        top_input.reshape(tcells, tc), smooth_weight, fine_lateral, mid_lateral, top_lateral,
    )))
    gf, gm, gt, kg, ml, tl = pl.pallas_call(
        put_out,
        out_shape=wide + final,
        in_specs=[inner] * 5,
        out_specs=[hbm] * 6,
        scratch_shapes=[dma((6,))],
        compiler_params=pltpu.CompilerParams(vmem_limit_bytes=8 * 1024 * 1024),
    )(*between)
    return (
        gf.reshape(fine_input.shape), gm.reshape(mid_input.shape),
        gt.reshape(top_input.shape), kg, ml, tl,
    )


def body(nr, *args):
    fine_level, out_grad, fine_input, mid_input, top_input = args[:5]
    dp = lax.axis_size("dp")
    chips = dp // 2
    nx = max((n for n in range(1, chips + 1) if chips % n == 0 and n * n <= chips), default=1)
    images, strip, width, chans = out_grad.shape
    rows = 9 * chans + fine_input.shape[-1]
    coarse = mid_input.shape[-1] + top_input.shape[-1]
    fits = (
        dp % 2 == 0 and images == 1 and nr > 1 and chips > nx > 1 and chips // nx > 2
        and rows % (dp * nr * 16) == 0 and coarse % (dp * 16) == 0
        and strip % 4 == 0 and strip >= 8 and width % 64 == 0 and chans % 128 == 0
    )
    if not fits:
        return plain_body(*args)
    return kernel_body(chips // nx, nx, nr, *args)


def solution(mesh):
    placed = (
        P("dp", "rows", None, None),
        P("dp", "rows", None, None),
        P("dp", "rows", None, None),
        P("dp", None, None, "rows"),
        P("dp", None, None, "rows"),
        P(),
        P(),
        P("rows", None),
        P("rows", None),
    )
    return jax.shard_map(
        functools.partial(body, mesh.shape["rows"]),
        mesh=mesh,
        in_specs=placed,
        out_specs=(
            P("dp", "rows", None, None),
            P("dp", None, None, "rows"),
            P("dp", None, None, "rows"),
            P("dp", None),
            P("rows", None),
            P("rows", None),
        ),
        check_vma=False,
    )
```

```python
import functools

import jax
import jax.numpy as jnp
from jax import lax
from jax.experimental import pallas as pl
from jax.experimental.pallas import tpu as pltpu
from jax.sharding import PartitionSpec as P

BF = jnp.bfloat16
F32 = jnp.float32
MESH = pl.DeviceIdType.MESH


def with_halo(value, sides, width):
    for axis, dim in sides:
        count, length = (lax.axis_size(axis), value.shape[dim])
        up = [(i, (i + 1) % count) for i in range(count - 1)]
        down = [(j, i) for i, j in up]
        last = lax.slice_in_dim(value, length - width, length, axis=dim)
        leading = lax.slice_in_dim(value, 0, width, axis=dim)
        before = lax.ppermute(last, axis, up)
        after = lax.ppermute(leading, axis, down)
        value = jnp.concatenate([before, value, after], axis=dim)
    return value


def pool_two(field):
    images, rows_n, cols_n, chans = field.shape
    return field.reshape(images, rows_n // 2, 2, cols_n // 2, 2, chans).sum(axis=(2, 4))


def contract_last(left, right):
    return lax.dot_general(
        left, right, (((1,), (1,)), ((), ())), preferred_element_type=jnp.float32
    )


def contract_first(left, right):
    return lax.dot_general(
        left, right, (((0,), (0,)), ((), ())), preferred_element_type=jnp.float32
    )


def plain_body(
    fine_level,
    out_grad,
    fine_input,
    mid_input,
    top_input,
    smooth_weight,
    fine_lateral,
    mid_lateral,
    top_lateral,
):
    images, strip, width, chans = out_grad.shape
    cells = images * strip * width
    rimmed = with_halo(out_grad, (("rows", 1),), 1)
    rimmed = jnp.pad(rimmed, ((0, 0), (0, 0), (1, 1), (0, 0)))
    fine_flat = fine_level.reshape(cells, chans)
    level_grad = jnp.zeros((cells, chans), jnp.float32)
    pieces = []
    for tap_a in range(3):
        for tap_b in range(3):
            shifted = rimmed[
                :, 2 - tap_a : 2 - tap_a + strip, 2 - tap_b : 2 - tap_b + width, :
            ].reshape(cells, chans)
            level_grad = level_grad + contract_last(shifted, smooth_weight[tap_a, tap_b])
            pieces.append(contract_first(fine_flat, shifted))
    fine_grad = level_grad.astype(jnp.bfloat16)
    grad_fine = (
        contract_last(fine_grad, fine_lateral)
        .astype(jnp.bfloat16)
        .reshape(images, strip, width, -1)
    )
    pieces.append(contract_first(fine_input.reshape(cells, -1), fine_grad))
    kernel_term = jnp.concatenate(pieces, axis=0)
    share = lax.psum_scatter(kernel_term, "dp", scatter_dimension=0, tiled=True)
    kernel_grads = lax.psum(share, "rows")
    pooled = pool_two(level_grad.reshape(images, strip, width, chans)).astype(jnp.bfloat16)
    mid_grad = lax.all_gather(pooled, "rows", axis=1, tiled=True)
    top_grad = pool_two(mid_grad.astype(jnp.float32)).astype(jnp.bfloat16)
    mid_flat = mid_grad.reshape(-1, chans)
    top_flat = top_grad.reshape(-1, chans)
    grad_mid = contract_last(mid_flat, mid_lateral).astype(jnp.bfloat16).reshape(mid_input.shape)
    grad_top = contract_last(top_flat, top_lateral).astype(jnp.bfloat16).reshape(top_input.shape)
    mid_term = contract_first(mid_input.reshape(mid_flat.shape[0], -1), mid_flat)
    top_term = contract_first(top_input.reshape(top_flat.shape[0], -1), top_flat)
    midlat_grad, toplat_grad = lax.psum((mid_term, top_term), "dp")
    return (grad_fine, grad_mid, grad_top, kernel_grads, midlat_grad, toplat_grad)


def rows_of(start, size, step):
    return pl.ds(pl.multiple_of(start, step), size)


def fused(
    nz, nx, nr, strip, width,
    fl_h, og_h, fi_h, mi_h, ti_h, w_h, lf_h, lm_h, lt_h,
    gf_h, gm_h, gt_h, kf_h, ga_h,
    og, fine, fin, mid_in, top_in, wcat, lat_f, lat_m, lat_t,
    halo, taps, ftr, acc, kacc, fg, pool_f, midg, topf, topg,
    kgb, ra, sb, rb, tb, rc, kf,
    ct, rca, sc, rcs, gath,
    in_sem, w_sem, halo_s, halo_r, mid_s, mid_r,
    a_s, a_r, b_s, b_r, c_s, c_r, d_s, d_r,
    ca_s, ca_r, cs_s, cs_r, cg_s, cg_r, cc_s, cc_r, relay,
):
    chips = nz * nx
    d = lax.axis_index("dp")
    r = lax.axis_index("rows")
    core = lax.rem(d, 2)
    q = d // 2
    x = lax.rem(q, nx)
    z = q // nx
    other = 1 - core
    sibling = (q * 2 + other, r)
    cells, chans = og.shape
    share = kf.shape[0]
    part = share // nr

    def dev(z1, x1, r1):
        return ((z1 * nx + x1) * 2 + core, r1)

    def remote(src, dst, ss, rs, to):
        return pltpu.make_async_remote_copy(
            src_ref=src, dst_ref=dst, send_sem=ss, recv_sem=rs,
            device_id=to, device_id_type=MESH,
        )

    loads = []
    for n, (src, dst) in enumerate(
        ((og_h, og), (fl_h, fine.at[pl.ds(width, cells)]), (fi_h, fin), (lf_h, lat_f),
         (mi_h, mid_in), (ti_h, top_in), (lm_h, lat_m), (lt_h, lat_t))
    ):
        loads.append(pltpu.make_async_copy(src, dst, in_sem.at[n]))
    wloads = []
    for a in range(3):
        for b in range(3):
            wloads.append(pltpu.make_async_copy(
                w_h.at[a, b], wcat.at[a, :, b * chans:(b + 1) * chans], w_sem.at[3 * a + b]
            ))
    loads[0].start()

    barrier = pltpu.get_barrier_semaphore()
    plane = [(i, j) for i in range(nx) for j in range(nr) if (i, j) != (0, 0)]
    near = []
    for low_end, high_end, before, after in (
        (z > 0, z < nz - 1, dev(jnp.maximum(z - 1, 0), x, r), dev(jnp.minimum(z + 1, nz - 1), x, r)),
        (x > 0, x < nx - 1, dev(z, jnp.maximum(x - 1, 0), r), dev(z, jnp.minimum(x + 1, nx - 1), r)),
        (r > 0, r < nr - 1, dev(z, x, jnp.maximum(r - 1, 0)), dev(z, x, jnp.minimum(r + 1, nr - 1))),
    ):
        near += [(low_end, before), (high_end, after)]
    nearby = sum(there.astype(jnp.int32) for there, _ in near)

    def greet(sem):
        for there, to in near:
            @pl.when(there)
            def _():
                pl.semaphore_signal(sem, inc=1, device_id=to, device_id_type=MESH)

    def hear(k):
        pl.semaphore_wait(relay.at[k], nearby)
        if k + 1 < relays:
            greet(relay.at[k + 1])

    relays = relay.shape[0]
    pl.semaphore_signal(barrier, inc=1, device_id=sibling, device_id_type=MESH)
    greet(barrier)

    loads[1].start()
    for cp in wloads:
        cp.start()
    for cp in loads[2:]:
        cp.start()

    top_rim, low_rim = pl.ds(0, width), pl.ds((strip + 1) * width, width)
    taps[top_rim, :] = jnp.zeros((width, 3 * chans), BF)
    taps[low_rim, :] = jnp.zeros((width, 3 * chans), BF)
    fine[top_rim, :] = jnp.zeros((width, chans), BF)
    fine[low_rim, :] = jnp.zeros((width, chans), BF)

    col = lax.broadcasted_iota(jnp.int32, (width, chans), 0)

    def spread(value, here):
        wide = value.astype(F32)
        after = jnp.where(col == width - 1, 0.0, pltpu.roll(wide, width - 1, 0))
        before = jnp.where(col == 0, 0.0, pltpu.roll(wide, 1, 0))
        taps[here, 0:chans] = after.astype(BF)
        taps[here, chans:2 * chans] = value
        taps[here, 2 * chans:3 * chans] = before.astype(BF)

    loads[0].wait()
    def spread_row(y, carry):
        spread(og[rows_of(y * width, width, width), :], rows_of((y + 1) * width, width, width))
        return carry

    lax.fori_loop(0, strip, spread_row, 0)
    loads[1].wait()
    wide_t = fine[...].T
    ftr[pl.ds(0, chans), :] = wide_t[:, 0:cells]
    ftr[pl.ds(chans, chans), :] = fine[pl.ds(width, cells), :].T
    ftr[pl.ds(2 * chans, chans), :] = wide_t[:, 2 * width:2 * width + cells]

    pl.semaphore_wait(barrier, nearby + 1)
    greet(relay.at[0])
    down = remote(og.at[pl.ds(cells - width, width)], halo.at[0], halo_s.at[0], halo_r.at[0],
                  (d, lax.rem(r + 1, nr)))
    up = remote(og.at[pl.ds(0, width)], halo.at[1], halo_s.at[1], halo_r.at[1],
                (d, lax.rem(r + nr - 1, nr)))

    @pl.when(r < nr - 1)
    def _():
        down.start()

    @pl.when(r > 0)
    def _():
        up.start()

    for cp in wloads:
        cp.wait()

    level = contract_last(taps[pl.ds(2 * width, cells), :], wcat[0])
    level += contract_last(taps[pl.ds(width, cells), :], wcat[1])
    level += contract_last(taps[pl.ds(0, cells), :], wcat[2])
    acc[...] = level
    fg[...] = level.astype(BF)

    hear(0)
    half = width // 2
    mine = cells // 4
    lanes = [pl.ds(v * 128, 128) for v in range(chans // 128)]

    def pool(y0, count):
        for y in range(count):
            at = 2 * (y0 + y) * width
            pair = acc[rows_of(at, width, width), :] + acc[rows_of(at + width, width, width), :]
            for v in range(chans // 128):
                pool_f[v, pl.ds(y * width, width), :] = pair[:, v * 128:(v + 1) * 128]
        for v, lane in enumerate(lanes):
            midg[r, rows_of(y0 * half, count * half, 16), lane] = (
                pool_f[v, pl.ds(0, count * half, stride=2), :]
                + pool_f[v, pl.ds(1, count * half, stride=2), :]
            ).astype(BF)

    mrows = strip // 2
    pool(0, mrows)
    rims = [r] if nr == 2 else [0, 1]
    start = r if nr == 2 else 1
    count = mrows - len(rims)
    mids = []

    def send_mid(e, y0, count):
        here = midg.at[r, rows_of(y0 * half, count * half, 16)]
        for j in range(1, nr):
            cp = remote(here, here, mid_s.at[j - 1, e], mid_r.at[j - 1, e],
                        (d, lax.rem(r + j, nr)))
            cp.start()
            mids.append(cp)

    send_mid(0, start, count)
    inner = rows_of(start * width, cells - len(rims) * width, width)

    def ktap(b, carry):
        got = jnp.dot(
            ftr[...], taps[pl.ds(width, cells), pl.ds(pl.multiple_of(b * chans, 128), chans)],
            preferred_element_type=F32,
        )
        for a in range(3):
            kgb[rows_of((3 * a + b) * chans, chans, 16), :] = got[a * chans:(a + 1) * chans].astype(BF)
        kacc[0, rows_of(b * chans, chans, 16), :] = got[0:chans]
        kacc[1, rows_of(b * chans, chans, 16), :] = got[2 * chans:3 * chans]
        return carry

    lax.fori_loop(0, 3, ktap, 0)

    hear(1)
    loads[2].wait()
    fsum = jnp.dot(fin[inner, :].T, fg[inner, :], preferred_element_type=F32)

    @pl.when(r > 0)
    def _():
        down.wait_recv()

    @pl.when(r < nr - 1)
    def _():
        up.wait_recv()

    if nr > 2:
        @pl.when(r == 0)
        def _():
            halo[0] = jnp.zeros_like(halo[0])

        @pl.when(r == nr - 1)
        def _():
            halo[1] = jnp.zeros_like(halo[1])

    def mend(n, e):
        rim = rows_of((1 - e) * (strip + 1) * width, width, width)
        edge = rows_of((1 - e) * (cells - width), width, width)
        mate = rows_of((1 - e) * (cells - width) + width, width, width)
        y0 = (1 - e) * (mrows - 1)
        spread(halo[1 - e], rim)
        acc[edge, :] += contract_last(taps[rim, :], wcat[2 * e])
        pool(y0, 1)
        send_mid(1 + n, y0, 1)
        fg[edge, :] = acc[edge, :].astype(BF)
        more = jnp.dot(fine[mate, :].T, taps[rim, :], preferred_element_type=F32)
        for b in range(3):
            kgb[rows_of((6 * e + b) * chans, chans, 16), :] = (
                kacc[e, pl.ds(b * chans, chans), :] + more[:, b * chans:(b + 1) * chans]
            ).astype(BF)
        return edge

    for n, e in enumerate(rims):
        edge = mend(n, e)
        fsum += jnp.dot(fin[edge, :].T, fg[edge, :], preferred_element_type=F32)
    kgb[pl.ds(9 * chans, fin.shape[1]), :] = fsum.astype(BF)

    for k in range(2, relays):
        hear(k)
    low = z < nz // 2
    far = []
    for k in range(nz - 1):
        down_z = nz - 1 - k
        zt = jnp.where(low, jnp.where(down_z > z, down_z, down_z - 1), jnp.where(k < z, k, k + 1))
        far.append(zt)
    far.append(z)
    firsts = []
    for zt in far:
        for i in range(nx):
            n = zt * nx + i
            cp = remote(kgb.at[rows_of((2 * n + other) * share, share, 16)], ra.at[n],
                        a_s.at[n], a_r.at[n], sibling)
            cp.start()
            firsts.append((n, cp))

    loads[3].wait()
    gf_h[...] = contract_last(fg[...], lat_f[...]).astype(BF)

    seconds = []

    def sum_group(g):
        for n, cp in firsts[g * nx:(g + 1) * nx]:
            cp.wait_recv()
            sb[n] = (
                kgb[rows_of((2 * n + core) * share, share, 16), :].astype(F32) + ra[n].astype(F32)
            ).astype(BF)

    def send_group(g):
        row = []
        for n, (i, j) in enumerate(plane):
            xt, rt = lax.rem(x + i, nx), lax.rem(r + j, nr)
            cp = remote(sb.at[far[g] * nx + xt, rows_of(rt * part, part, 16)], rb.at[n, g],
                        b_s.at[n, g], b_r.at[n, g], dev(z, xt, rt))
            cp.start()
            row.append(cp)
        seconds.append((g, far[g], row))

    ahead = nz - 1
    for g in range(ahead):
        sum_group(g)
        send_group(g)

    for cp in mids:
        cp.wait_recv()
    loads[4].wait()
    loads[5].wait()
    hw = half
    for t in range(nr):
        for y in range(strip // 4):
            pair = (
                midg[t, pl.ds(2 * y * hw, hw), :].astype(F32)
                + midg[t, pl.ds((2 * y + 1) * hw, hw), :].astype(F32)
            )
            for v in range(chans // 128):
                topf[v, pl.ds((t * (strip // 4) + y) * hw, hw), :] = pair[:, v * 128:(v + 1) * 128]
    tops = topg.shape[0]
    for v, lane in enumerate(lanes):
        topg[:, lane] = (
            topf[v, pl.ds(0, tops, stride=2), :] + topf[v, pl.ds(1, tops, stride=2), :]
        ).astype(BF)
    mflat = midg[...].reshape(nr * mine, chans)
    mc, tc = mid_in.shape[1], top_in.shape[1]
    ct[pl.ds(0, mc), :] = jnp.dot(
        mid_in[...].T, mflat, preferred_element_type=F32).astype(BF)
    ct[pl.ds(mc, tc), :] = jnp.dot(
        top_in[...].T, topg[...], preferred_element_type=F32).astype(BF)
    per = sc.shape[0]
    chunk = per // chips
    cfirst = remote(ct.at[rows_of(other * per, per, 16)], rca, ca_s, ca_r, sibling)
    cfirst.start()
    for g in range(ahead, nz):
        sum_group(g)
    cfirst.wait_recv()
    sc[...] = (
        ct[rows_of(core * per, per, 16), :].astype(F32) + rca[...].astype(F32)
    ).astype(BF)
    cscat = []
    for k in range(1, chips):
        to = lax.rem(q + k, chips)
        cp = remote(sc.at[rows_of(to * chunk, chunk, 16)], rcs.at[k - 1],
                    cs_s.at[k - 1], cs_r.at[k - 1], (to * 2 + core, r))
        cp.start()
        cscat.append(cp)

    for g in range(ahead, nz):
        send_group(g)

    loads[6].wait()
    gm_h[...] = contract_last(mflat, lat_m[...]).astype(BF)
    loads[7].wait()
    gt_h[...] = contract_last(topg[...], lat_t[...]).astype(BF)

    thirds = []
    for g, zt, row in seconds[:-1]:
        total = sb[zt * nx + x, rows_of(r * part, part, 16), :].astype(F32)
        for n, cp in enumerate(row):
            cp.wait_recv()
            total += rb[n, g].astype(F32)
        tb[g] = total.astype(BF)
        cp = remote(tb.at[g], rc.at[z], c_s.at[g], c_r.at[z], dev(zt, x, r))
        cp.start()
        thirds.append(cp)

    total = sc[rows_of(q * chunk, chunk, 16), :].astype(F32)
    for k in range(1, chips):
        cscat[k - 1].wait_recv()
        total += rcs[k - 1].astype(F32)
    place = core * per + q * chunk
    gath[rows_of(place, chunk, 16), :] = total.astype(BF)

    def hand_over(k):
        held = gath.at[rows_of(core * per + lax.rem(q + chips - k, chips) * chunk, chunk, 16)]
        return remote(held, held, cc_s.at[k], cc_r.at[k], sibling)

    cgath = []
    for k in range(1, chips):
        here = rows_of(place, chunk, 16)
        cp = remote(gath.at[here], gath.at[here], cg_s.at[k - 1], cg_r.at[k - 1],
                    (lax.rem(q + k, chips) * 2 + core, r))
        cp.start()
        cgath.append(cp)
    hand_over(0).start()

    total = sb[z * nx + x, rows_of(r * part, part, 16), :].astype(F32)
    for n, cp in enumerate(seconds[-1][2]):
        cp.wait_recv()
        total += rb[n, nz - 1].astype(F32)
    for k in range(1, nz):
        source = lax.rem(z + k, nz)
        remote(tb.at[0], rc.at[source], c_s.at[0], c_r.at[source], dev(source, x, r)).wait_recv()
        total += rc[source].astype(F32)
    spot = rows_of(r * part, part, 16)
    kf[spot, :] = total.astype(BF)
    lasts = []
    for j in range(1, nr):
        cp = remote(kf.at[spot], kf.at[spot], d_s.at[j - 1], d_r.at[j - 1],
                    (d, lax.rem(r + j, nr)))
        cp.start()
        lasts.append(cp)

    for k in range(1, chips):
        cgath[k - 1].wait_recv()
        hand_over(k).start()
    for cp in lasts:
        cp.wait_recv()
    kf_h[...] = kf[...].astype(F32)
    block = rows_of(core * per, per, 16)
    ga_h[block, :] = gath[block, :].astype(F32)
    for k in range(chips):
        hand_over(k).wait_recv()
    rest = rows_of(other * per, per, 16)
    ga_h[rest, :] = gath[rest, :].astype(F32)

    @pl.when(r < nr - 1)
    def _():
        down.wait_send()

    @pl.when(r > 0)
    def _():
        up.wait_send()

    sent = mids + [cp for _, cp in firsts] + [cfirst] + cscat + cgath + thirds + lasts + [hand_over(k) for k in range(chips)]
    for _, _, row in seconds:
        sent += row
    for cp in sent:
        cp.wait_send()


def put_out(gf_i, gm_i, gt_i, kg_i, ga_i, gf_o, gm_o, gt_o, kg_o, ml_o, tl_o, out_sem):
    mc = ml_o.shape[0]
    pairs = (
        (ga_i.at[pl.ds(mc, tl_o.shape[0])], tl_o), (gf_i, gf_o), (ga_i.at[pl.ds(0, mc)], ml_o),
        (gm_i, gm_o), (kg_i, kg_o), (gt_i, gt_o),
    )
    stores = [pltpu.make_async_copy(src, dst, out_sem.at[n]) for n, (src, dst) in enumerate(pairs)]
    for cp in stores:
        cp.start()
    for cp in stores:
        cp.wait()


def kernel_body(nz, nx, nr, fine_level, out_grad, fine_input, mid_input, top_input,
                smooth_weight, fine_lateral, mid_lateral, top_lateral):
    _, strip, width, chans = out_grad.shape
    cells = strip * width
    cin = fine_input.shape[-1]
    mc, tc = mid_input.shape[-1], top_input.shape[-1]
    mcells = mid_input.shape[1] * mid_input.shape[2]
    tcells = top_input.shape[1] * top_input.shape[2]
    chips = nz * nx
    rows = 9 * chans + cin
    share = rows // (2 * chips)
    part = share // nr
    per = (mc + tc) // 2
    chunk = per // chips
    npl = nx * nr - 1
    dma = pltpu.SemaphoreType.DMA
    vm = pltpu.VMEM
    scratch = [
        vm((cells, chans), BF), vm(((strip + 2) * width, chans), BF), vm((cells, cin), BF),
        vm((mcells, mc), BF), vm((tcells, tc), BF), vm((3, chans, 3 * chans), BF),
        vm((cin, chans), BF), vm((mc, chans), BF), vm((tc, chans), BF),
        vm((2, width, chans), BF), vm(((strip + 2) * width, 3 * chans), BF),
        vm((3 * chans, cells), BF), vm((cells, chans), F32), vm((2, 3 * chans, chans), F32), vm((cells, chans), BF), vm((chans // 128, cells // 2, 128), F32),
        vm((nr, cells // 4, chans), BF), vm((chans // 128, mcells // 2, 128), F32), vm((tcells, chans), BF),
        vm((rows, chans), BF), vm((chips, share, chans), BF), vm((chips, share, chans), BF),
        vm((npl, nz, part, chans), BF), vm((nz - 1, part, chans), BF),
        vm((nz, part, chans), BF), vm((share, chans), BF),
        vm((2 * per, chans), BF), vm((per, chans), BF), vm((per, chans), BF),
        vm((chips - 1, chunk, chans), BF), vm((2 * per, chans), BF),
        dma((8,)), dma((9,)), dma((2,)), dma((2,)), dma((nr - 1, 3)), dma((nr - 1, 3)),
        dma((chips,)), dma((chips,)), dma((npl, nz)), dma((npl, nz)),
        dma((nz - 1,)), dma((nz,)), dma((nr - 1,)), dma((nr - 1,)),
        dma(()), dma(()), dma((chips - 1,)), dma((chips - 1,)),
        dma((chips - 1,)), dma((chips - 1,)), dma((chips,)), dma((chips,)),
        pltpu.SemaphoreType.REGULAR((max(nz + nx, nx + nr) - 3,)),
    ]
    hbm = pl.BlockSpec(memory_space=pltpu.HBM)
    inner = pl.BlockSpec(memory_space=pltpu.VMEM)
    wide = [
        jax.ShapeDtypeStruct((cells, cin), BF), jax.ShapeDtypeStruct((mcells, mc), BF),
        jax.ShapeDtypeStruct((tcells, tc), BF),
    ]
    held = [jax.ShapeDtypeStruct((share, chans), F32), jax.ShapeDtypeStruct((2 * per, chans), F32)]
    final = [
        jax.ShapeDtypeStruct((share, chans), F32), jax.ShapeDtypeStruct((mc, chans), F32),
        jax.ShapeDtypeStruct((tc, chans), F32),
    ]
    whole = 67043328
    between = pl.pallas_call(
        functools.partial(fused, nz, nx, nr, strip, width),
        out_shape=[pltpu.VMEM(o.shape, o.dtype) for o in wide + held],
        in_specs=[hbm] * 9,
        out_specs=[inner] * 5,
        scratch_shapes=scratch,
        compiler_params=pltpu.CompilerParams(
            collective_id=0, has_side_effects=True, vmem_limit_bytes=48 * 1024 * 1024
        ),
    )(*(pltpu.with_memory_space_constraint(value, pltpu.HBM) for value in (
        fine_level.reshape(cells, chans), out_grad.reshape(cells, chans),
        fine_input.reshape(cells, cin), mid_input.reshape(mcells, mc),
        top_input.reshape(tcells, tc), smooth_weight, fine_lateral, mid_lateral, top_lateral,
    )))
    gf, gm, gt, kg, ml, tl = pl.pallas_call(
        put_out,
        out_shape=wide + final,
        in_specs=[inner] * 5,
        out_specs=[hbm] * 6,
        scratch_shapes=[dma((6,))],
        compiler_params=pltpu.CompilerParams(vmem_limit_bytes=8 * 1024 * 1024),
    )(*between)
    return (
        gf.reshape(fine_input.shape), gm.reshape(mid_input.shape),
        gt.reshape(top_input.shape), kg, ml, tl,
    )


def body(nr, *args):
    fine_level, out_grad, fine_input, mid_input, top_input = args[:5]
    dp = lax.axis_size("dp")
    chips = dp // 2
    nx = max((n for n in range(1, chips + 1) if chips % n == 0 and n * n <= chips), default=1)
    images, strip, width, chans = out_grad.shape
    rows = 9 * chans + fine_input.shape[-1]
    coarse = mid_input.shape[-1] + top_input.shape[-1]
    fits = (
        dp % 2 == 0 and images == 1 and nr > 1 and chips > nx > 1 and chips // nx > 2
        and rows % (dp * nr * 16) == 0 and coarse % (dp * 16) == 0
        and strip % 4 == 0 and strip >= 8 and width % 64 == 0 and chans % 128 == 0
    )
    if not fits:
        return plain_body(*args)
    return kernel_body(chips // nx, nx, nr, *args)


def solution(mesh):
    placed = (
        P("dp", "rows", None, None),
        P("dp", "rows", None, None),
        P("dp", "rows", None, None),
        P("dp", None, None, "rows"),
        P("dp", None, None, "rows"),
        P(),
        P(),
        P("rows", None),
        P("rows", None),
    )
    return jax.shard_map(
        functools.partial(body, mesh.shape["rows"]),
        mesh=mesh,
        in_specs=placed,
        out_specs=(
            P("dp", "rows", None, None),
            P("dp", None, None, "rows"),
            P("dp", None, None, "rows"),
            P("dp", None),
            P("rows", None),
            P("rows", None),
        ),
        check_vma=False,
    )
```
